32 devices in a mesh: dp: 4 (over x, y), tp: 8 (over z, core).
Axes of the slice: x: 2, y: 2, z: 4, core: 2. Of those that a mesh axis runs over, the one named last changes fastest.
Arguments:
- x: bfloat16 [8192, 4096], P(('dp', 'tp')), parts along dimension 0
- w_gate: bfloat16 [4096, 10240], P(None, 'tp')
- w_up: bfloat16 [4096, 10240], P(None, 'tp')
- w_down: bfloat16 [10240, 4096], P('tp')
Outputs:
- output: bfloat16 [8192, 4096], P(('dp', 'tp')), parts along dimension 0
There are 4 independent parts. The reference program is written for one: setup_inputs(seed, part) draws one part's arguments, and reference() takes and returns one part's arrays. A program takes and returns all parts, laid end to end along the dimension named above; an argument that names none is the same for every part.
All inputs are finite; a program needn't handle non-finite values.
Results may differ from the reference program's by a relative error of at most 0.016.
Values are sent between devices in bfloat16 or wider.
A program may use at most 2 GiB of HBM per device.

```python
import jax
import jax.numpy as jnp

ROWS = 2048
D = 4096
FF = 10240


def setup_inputs(seed: int = 0, part: int = 0) -> dict:
    kx, kg, ku, kd = jax.random.split(jax.random.key(seed), 4)
    drawn = {
        "x": jax.random.normal(jax.random.fold_in(kx, part), (ROWS, D), jnp.float32),
        "w_gate": jax.random.normal(kg, (D, FF), jnp.float32) * D**-0.5,
        "w_up": jax.random.normal(ku, (D, FF), jnp.float32) * D**-0.5,
        "w_down": jax.random.normal(kd, (FF, D), jnp.float32) * FF**-0.5,
    }
    return {k: v.astype(jnp.bfloat16) for k, v in drawn.items()}


def reference(x, w_gate, w_up, w_down):
    gate = jnp.dot(x, w_gate, preferred_element_type=jnp.float32)
    up = jnp.dot(x, w_up, preferred_element_type=jnp.float32)
    hidden = (jax.nn.gelu(gate) * up).astype(jnp.bfloat16)
    return jnp.dot(hidden, w_down, preferred_element_type=jnp.float32).astype(jnp.bfloat16)
```

```python
import functools

import jax
import jax.numpy as jnp
from jax import lax
from jax.experimental import pallas as pl
from jax.experimental.pallas import tpu as pltpu
from jax.sharding import PartitionSpec as P

MESH = pl.DeviceIdType.MESH
F32, BF16 = jnp.float32, jnp.bfloat16

CHUNKS = 2
PIECES = 8
RING = 8
LAG = 2
UNIT = CHUNKS * PIECES


def kernel(
    x, wg, wu, wd, y, tm, ts, vwg, vwu, vwd, xb, hid,
    own1, sib1, stg1, own2, sib2, stg2, rse, rsi,
    w_sem, x_sem, y_sem, tm_recv, ts_recv, ti_send, te_send, ts_send,
    d1_send, d1_recv, d2_send, d2_recv, rse_send, rse_recv, rsi_send, rsi_recv,
):
    me = lax.axis_index("tp")
    chip, core = me // 2, lax.rem(me, 2)
    is_end = jnp.logical_or(chip == 0, chip == 3)
    sibling = me + 1 - 2 * core
    inward = jnp.where(chip < 2, 2, -2)
    to_in, to_out = me + inward, me - inward
    rows = x.shape[0] // CHUNKS
    width = y.shape[1] // PIECES
    tile = min(256, vwg.shape[1])
    tiles = vwg.shape[1] // tile

    weights = [pltpu.make_async_copy(s, d, w_sem.at[i]) for i, (s, d) in enumerate(((wg, vwg), (wu, vwu), (wd, vwd)))]
    for w in weights:
        w.start()

    barrier = pltpu.get_barrier_semaphore()
    pl.semaphore_signal(barrier, inc=1, device_id={"tp": sibling}, device_id_type=MESH)
    pl.semaphore_signal(barrier, inc=1, device_id={"tp": to_in}, device_id_type=MESH)

    @pl.when(is_end)
    def _():
        pl.semaphore_wait(barrier, 2)

    @pl.when(jnp.logical_not(is_end))
    def _():
        pl.semaphore_signal(barrier, inc=1, device_id={"tp": to_out}, device_id_type=MESH)
        pl.semaphore_wait(barrier, 3)

    def remote(src, dst, send, recv, device):
        return pltpu.make_async_remote_copy(
            src_ref=src, dst_ref=dst, send_sem=send, recv_sem=recv, device_id={"tp": device}, device_id_type=MESH
        )

    def x_rows(j):
        return x.at[pl.ds(pl.multiple_of(j * rows, rows), rows), :]

    def own_to_in(j):
        slot = jnp.where(is_end, 0, CHUNKS) + j
        return remote(x_rows(j), tm.at[slot], ti_send.at[j], tm_recv.at[slot], to_in)

    def own_to_out(j):
        return remote(x_rows(j), tm.at[j], te_send.at[j], tm_recv.at[j], to_out)

    def own_to_sibling(j):
        return remote(x_rows(j), ts.at[j], ts_send.at[j], ts_recv.at[j], sibling)

    def on_to_in(j):
        slot = 2 * CHUNKS + j
        return remote(tm.at[j], tm.at[slot], ti_send.at[CHUNKS + j], tm_recv.at[slot], to_in)

    def on_to_out(a):
        return remote(tm.at[a], tm.at[a], te_send.at[a], tm_recv.at[a], to_out)

    def on_to_sibling(a):
        c = CHUNKS + a
        return remote(tm.at[a], ts.at[c], ts_send.at[c], ts_recv.at[c], sibling)

    def wait_arrival(a):
        on_to_out(a).wait_recv()

    def load(c, mine):
        pltpu.make_async_remote_copy(
            src_ref=ts.at[c], dst_ref=ts.at[c], send_sem=ts_send.at[c], recv_sem=ts_recv.at[c],
            device_id={"tp": sibling}, device_id_type=MESH,
        ).wait_recv()
        first = pltpu.make_async_copy(mine, xb.at[pl.ds(0, rows)], x_sem.at[0])
        second = pltpu.make_async_copy(ts.at[c], xb.at[pl.ds(rows, rows)], x_sem.at[1])
        first.start()
        second.start()
        first.wait()
        second.wait()

    def hidden_tile(c, i):
        columns = pl.ds(pl.multiple_of(i * tile, tile), tile)
        gate = jnp.dot(xb[...], vwg[:, columns], preferred_element_type=F32)
        up = jnp.dot(xb[...], vwu[:, columns], preferred_element_type=F32)
        hid[c, :, columns] = (jax.nn.gelu(gate) * up).astype(BF16)

    def hidden(c):
        @pl.loop(0, tiles)
        def _(i):
            hidden_tile(c, i)

    def to_sibling(stg, sib, send, recv, k):
        s = lax.rem(k, RING)
        return remote(stg.at[s], sib.at[s], send.at[s], recv.at[s], sibling)

    def term(flow, k, c, n):
        own, sib, stg, send, recv = flow
        s = lax.rem(k, RING)

        @pl.when(k >= RING)
        def _():
            to_sibling(stg, sib, send, recv, k).wait_send()

        columns = pl.ds(pl.multiple_of(n * width, width), width)
        both = jnp.dot(hid[c], vwd[:, columns], preferred_element_type=F32)
        stg[s] = both[rows:].astype(BF16)
        own[s] = both[:rows]
        to_sibling(stg, sib, send, recv, k).start()

    def chip_sum(flow, k):
        own, sib, stg, send, recv = flow
        s = lax.rem(k, RING)
        to_sibling(stg, sib, send, recv, k).wait_recv()
        return own[s] + sib[s].astype(F32)

    def drain(flow):
        own, sib, stg, send, recv = flow

        @pl.loop(0, RING)
        def _(k):
            to_sibling(stg, sib, send, recv, k).wait_send()

    flow1 = (own1, sib1, stg1, d1_send, d1_recv)
    flow2 = (own2, sib2, stg2, d2_send, d2_recv)

    def end_sum_in(k):
        return remote(rse.at[k], rse.at[k], rse_send.at[k], rse_recv.at[k], to_in)

    def inner_sum_in(k):
        return remote(rse.at[k], rsi.at[k - UNIT], rse_send.at[k], rsi_recv.at[k - UNIT], to_in)

    def sum_out(k):
        return remote(rsi.at[k], rsi.at[k], rsi_send.at[k], rsi_recv.at[k], to_out)

    def result(k):
        j, n = lax.rem(k, UNIT) // PIECES, lax.rem(k, PIECES)
        place = y.at[pl.ds(pl.multiple_of(j * rows, rows), rows), pl.ds(pl.multiple_of(n * width, width), width)]
        return pltpu.make_async_copy(rsi.at[k], place, y_sem.at[lax.rem(k, UNIT)])

    for j in range(CHUNKS):
        own_to_in(j).start()

        @pl.when(jnp.logical_not(is_end))
        def _(j=j):
            own_to_out(j).start()

        own_to_sibling(j).start()

    weights[0].wait()
    weights[1].wait()

    @pl.loop(0, CHUNKS)
    def _(j):
        load(j, x_rows(j))
        hidden(j)

    weights[2].wait()

    @pl.when(is_end)
    def _():
        @pl.loop(0, 3 * CHUNKS)
        def _(a):
            wait_arrival(a)
            on_to_sibling(a).start()
            c = CHUNKS + a
            load(c, tm.at[a])
            hidden(c)

            @pl.loop(0, PIECES + LAG)
            def _(n):
                k = a * PIECES + n

                @pl.when(n < PIECES)
                def _():
                    term(flow1, k, c, n)

                @pl.when(n >= LAG)
                def _():
                    rse[k - LAG] = chip_sum(flow1, k - LAG).astype(BF16)
                    end_sum_in(k - LAG).start()

        @pl.loop(0, UNIT + LAG)
        def _(k):
            @pl.when(k < UNIT)
            def _():
                term(flow2, k, k // PIECES, lax.rem(k, PIECES))

            @pl.when(k >= LAG)
            def _():
                q = k - LAG
                total = chip_sum(flow2, q)
                sum_out(UNIT + q).wait_recv()
                rsi[UNIT + q] = (total + rsi[UNIT + q].astype(F32)).astype(BF16)
                result(UNIT + q).start()

        @pl.loop(0, 3 * UNIT)
        def _(k):
            end_sum_in(k).wait_send()

        @pl.loop(0, UNIT)
        def _(k):
            result(UNIT + k).wait()

    @pl.when(jnp.logical_not(is_end))
    def _():
        @pl.loop(0, CHUNKS)
        def _(j):
            wait_arrival(j)
            on_to_in(j).start()
            on_to_sibling(j).start()
            wait_arrival(CHUNKS + j)
            on_to_out(CHUNKS + j).start()
            on_to_sibling(CHUNKS + j).start()

            @pl.loop(0, 2)
            def _(u):
                a = u * CHUNKS + j
                load(CHUNKS + a, tm.at[a])
                hidden(CHUNKS + a)

        @pl.loop(2 * CHUNKS, 3 * CHUNKS)
        def _(a):
            wait_arrival(a)
            on_to_out(a).start()
            on_to_sibling(a).start()

            @pl.when(a < 3 * CHUNKS - 1)
            def _():
                load(CHUNKS + a, tm.at[a])
                hidden(CHUNKS + a)

        last = 4 * CHUNKS - 1

        def term1(k):
            term(flow1, k, (2 + k // UNIT) * CHUNKS + lax.rem(k, UNIT) // PIECES, lax.rem(k, PIECES))

        def term2(k):
            term(flow2, k, k // PIECES, lax.rem(k, PIECES))

        term1(0)

        @pl.loop(0, 2 * UNIT + LAG)
        def _(p):
            @pl.when(p < 2 * UNIT)
            def _():
                k = UNIT + p
                total = chip_sum(flow1, p)
                end_sum_in(k).wait_recv()
                rse[k] = (total + rse[k].astype(F32)).astype(BF16)
                inner_sum_in(k).start()

            @pl.when(p < 2 * UNIT - 1)
            def _():
                term1(p + 1)

            @pl.when(p >= LAG)
            def _():
                q = p - LAG
                total = chip_sum(flow2, q)
                sum_out(q).wait_recv()
                total = total + rsi[q].astype(F32)

                @pl.when(q < UNIT)
                def _():
                    end_sum_in(q).wait_recv()
                    rsi[q] = (total + rse[q].astype(F32)).astype(BF16)
                    result(q).start()

                @pl.when(q >= UNIT)
                def _():
                    rsi[q] = total.astype(BF16)
                    sum_out(q).start()

            @pl.when(jnp.logical_and(p >= LAG - 1, p < 2 * UNIT + LAG - 1))
            def _():
                term2(p - LAG + 1)

            @pl.when(p == 2)
            def _():
                load(last, tm.at[3 * CHUNKS - 1])

            @pl.when(jnp.logical_and(p >= 3, p < 3 + tiles))
            def _():
                hidden_tile(last, p - 3)

        @pl.loop(0, 2 * UNIT)
        def _(k):
            inner_sum_in(UNIT + k).wait_send()

        @pl.loop(0, UNIT)
        def _(k):
            sum_out(UNIT + k).wait_send()
            result(k).wait()

        @pl.loop(0, CHUNKS)
        def _(j):
            on_to_in(j).wait_send()
            own_to_out(j).wait_send()

        @pl.loop(CHUNKS, 3 * CHUNKS)
        def _(a):
            on_to_out(a).wait_send()

    drain(flow1)
    drain(flow2)

    @pl.loop(0, CHUNKS)
    def _(j):
        own_to_in(j).wait_send()
        own_to_sibling(j).wait_send()

    @pl.loop(0, 3 * CHUNKS)
    def _(a):
        on_to_sibling(a).wait_send()


def solution(mesh):
    def step(x, w_gate, w_up, w_down):
        n_rows, d = x.shape
        ff = w_gate.shape[1]
        rows, width = n_rows // CHUNKS, d // PIECES
        dma = pltpu.SemaphoreType.DMA
        out, _, _ = pl.pallas_call(
            kernel,
            out_shape=[
                jax.ShapeDtypeStruct((n_rows, d), BF16),
                jax.ShapeDtypeStruct((3 * CHUNKS, rows, d), BF16),
                jax.ShapeDtypeStruct((4 * CHUNKS, rows, d), BF16),
            ],
            in_specs=[pl.BlockSpec(memory_space=pltpu.HBM)] * 4,
            out_specs=[pl.BlockSpec(memory_space=pltpu.HBM)] * 3,
            scratch_shapes=[
                pltpu.VMEM((d, ff), BF16),
                pltpu.VMEM((d, ff), BF16),
                pltpu.VMEM((ff, d), BF16),
                pltpu.VMEM((2 * rows, d), BF16),
                pltpu.VMEM((4 * CHUNKS, 2 * rows, ff), BF16),
                *[
                    pltpu.VMEM((RING, rows, width), F32),
                    pltpu.VMEM((RING, rows, width), BF16),
                    pltpu.VMEM((RING, rows, width), BF16),
                ]
                * 2,
                pltpu.VMEM((3 * UNIT, rows, width), BF16),
                pltpu.VMEM((2 * UNIT, rows, width), BF16),
                dma((3,)),
                dma((2,)),
                dma((UNIT,)),
                dma((3 * CHUNKS,)),
                dma((4 * CHUNKS,)),
                dma((2 * CHUNKS,)),
                dma((3 * CHUNKS,)),
                dma((4 * CHUNKS,)),
                dma((RING,)),
                dma((RING,)),
                dma((RING,)),
                dma((RING,)),
                dma((3 * UNIT,)),
                dma((3 * UNIT,)),
                dma((2 * UNIT,)),
                dma((2 * UNIT,)),
            ],
            compiler_params=pltpu.CompilerParams(
                collective_id=0, has_side_effects=True, vmem_limit_bytes=66_000_000
            ),
            name="mlp_line",
        )(x, w_gate, w_up, w_down)
        return out

    return jax.shard_map(
        step,
        mesh=mesh,
        in_specs=(P(("dp", "tp"), None), P(None, "tp"), P(None, "tp"), P("tp", None)),
        out_specs=P(("dp", "tp"), None),
        check_vma=False,
    )
```

```python
import functools

import jax
import jax.numpy as jnp
from jax import lax
from jax.experimental import pallas as pl
from jax.experimental.pallas import tpu as pltpu
from jax.sharding import PartitionSpec as P

MESH = pl.DeviceIdType.MESH
F32, BF16 = jnp.float32, jnp.bfloat16

CHUNKS = 2
HALVES = 2
PARTS = CHUNKS * HALVES
PIECES = 8
RING = 8
AHEAD = 2
LAG = 2
HELD_END, HELD_INNER = 4, 2
UNIT = CHUNKS * PIECES
HELD = max(HELD_END, HELD_INNER)
FAR = 3


def kernel(
    x, wg, wu, wd, y, tm, ts, vwg, vwu, vwd, xb, acc, hid,
    own1, sib1, stg1, own2, sib2, stg2, rse, rsi,
    w_sem, x_sem, tm_recv, ts_recv, ti_send, te_send, ts_send,
    d1_send, d1_recv, d2_send, d2_recv, rse_send, rse_recv, rsi_send, rsi_recv,
):
    me = lax.axis_index("tp")
    chip, core = me // 2, lax.rem(me, 2)
    is_end = jnp.logical_or(chip == 0, chip == 3)
    sibling = me + 1 - 2 * core
    inward = jnp.where(chip < 2, 2, -2)
    to_in, to_out = me + inward, me - inward
    rows, half = x.shape[0] // CHUNKS, x.shape[1] // HALVES
    width = y.shape[1] // PIECES
    tile = min(256, vwg.shape[1])
    tiles = vwg.shape[1] // tile

    weights = [pltpu.make_async_copy(s, d, w_sem.at[i]) for i, (s, d) in enumerate(((wg, vwg), (wu, vwu), (wd, vwd)))]
    for w in weights:
        w.start()

    barrier = pltpu.get_barrier_semaphore()
    pl.semaphore_signal(barrier, inc=1, device_id={"tp": sibling}, device_id_type=MESH)
    pl.semaphore_signal(barrier, inc=1, device_id={"tp": to_in}, device_id_type=MESH)

    @pl.when(is_end)
    def _():
        pl.semaphore_wait(barrier, 2)

    @pl.when(jnp.logical_not(is_end))
    def _():
        pl.semaphore_signal(barrier, inc=1, device_id={"tp": to_out}, device_id_type=MESH)
        pl.semaphore_wait(barrier, 3)

    def remote(src, dst, send, recv, device):
        return pltpu.make_async_remote_copy(
            src_ref=src, dst_ref=dst, send_sem=send, recv_sem=recv, device_id={"tp": device}, device_id_type=MESH
        )

    def x_part(b):
        j, h = b // HALVES, lax.rem(b, HALVES)
        return x.at[pl.ds(pl.multiple_of(j * rows, rows), rows), pl.ds(pl.multiple_of(h * half, half), half)]

    def own_to_in(b):
        slot = jnp.where(is_end, 0, PARTS) + b
        return remote(x_part(b), tm.at[slot], ti_send, tm_recv.at[slot], to_in)

    def own_to_out(b):
        return remote(x_part(b), tm.at[b], te_send, tm_recv.at[b], to_out)

    def own_to_sibling(b):
        return remote(x_part(b), ts.at[b], ts_send, ts_recv.at[b], sibling)

    def on_to_in(b):
        slot = 2 * PARTS + b
        return remote(tm.at[b], tm.at[slot], ti_send, tm_recv.at[slot], to_in)

    def on_to_out(a):
        return remote(tm.at[a], tm.at[a], te_send, tm_recv.at[a], to_out)

    def on_to_sibling(a):
        c = PARTS + a
        return remote(tm.at[a], ts.at[c], ts_send, ts_recv.at[c], sibling)

    def wait_arrival(a):
        on_to_out(a).wait_recv()

    def wait_bytes(ref, count, sem):
        whole = ref.at[pl.ds(0, count)]
        pltpu.make_async_copy(whole, whole, sem).wait()

    def load(c, h, mine):
        theirs = ts.at[c * HALVES + h]
        remote(theirs, theirs, ts_send, ts_recv.at[c * HALVES + h], sibling).wait_recv()
        first = pltpu.make_async_copy(mine, xb.at[h, pl.ds(0, rows)], x_sem.at[0])
        second = pltpu.make_async_copy(theirs, xb.at[h, pl.ds(rows, rows)], x_sem.at[1])
        first.start()
        second.start()
        first.wait()
        second.wait()

    def product(weight, columns, h):
        return jnp.dot(xb[h], weight[pl.ds(h * half, half), columns], preferred_element_type=F32)

    def finish(c, columns, gate, up):
        hid[c, :, columns] = (jax.nn.gelu(gate) * up).astype(BF16)

    def hidden_tile(c, i):
        columns = pl.ds(pl.multiple_of(i * tile, tile), tile)
        gate = product(vwg, columns, 0) + product(vwg, columns, 1)
        up = product(vwu, columns, 0) + product(vwu, columns, 1)
        finish(c, columns, gate, up)

    def hidden_first():
        @pl.loop(0, tiles)
        def _(i):
            columns = pl.ds(pl.multiple_of(i * tile, tile), tile)
            acc[0, :, columns] = product(vwg, columns, 0)
            acc[1, :, columns] = product(vwu, columns, 0)

    def hidden_second(c):
        @pl.loop(0, tiles)
        def _(i):
            columns = pl.ds(pl.multiple_of(i * tile, tile), tile)
            gate = acc[0, :, columns] + product(vwg, columns, 1)
            up = acc[1, :, columns] + product(vwu, columns, 1)
            finish(c, columns, gate, up)

    def to_sibling(stg, sib, send, recv, k):
        s = lax.rem(k, RING)
        return remote(stg.at[s], sib.at[s], send.at[s], recv.at[s], sibling)

    def term(flow, k, c, n):
        own, sib, stg, send, recv = flow
        s = lax.rem(k, RING)

        @pl.when(k >= RING)
        def _():
            to_sibling(stg, sib, send, recv, k).wait_send()

        columns = pl.ds(pl.multiple_of(n * width, width), width)
        both = jnp.dot(hid[c], vwd[:, columns], preferred_element_type=F32)
        stg[s] = both[rows:].astype(BF16)
        own[s] = both[:rows]
        to_sibling(stg, sib, send, recv, k).start()

    def chip_sum(flow, k):
        own, sib, stg, send, recv = flow
        s = lax.rem(k, RING)
        to_sibling(stg, sib, send, recv, k).wait_recv()
        return own[s] + sib[s].astype(F32)

    def drain(flow):
        own, sib, stg, send, recv = flow

        @pl.loop(0, RING)
        def _(k):
            to_sibling(stg, sib, send, recv, k).wait_send()

    flow1 = (own1, sib1, stg1, d1_send, d1_recv)
    flow2 = (own2, sib2, stg2, d2_send, d2_recv)

    def end_sum_in(k):
        return remote(rse.at[k], rse.at[k], rse_send, rse_recv.at[k], to_in)

    def inner_sum_in(k):
        return remote(rse.at[k], rsi.at[k - UNIT], rse_send, rsi_recv.at[k - UNIT], to_in)

    def sum_out(k):
        return remote(rsi.at[k], rsi.at[k], rsi_send, rsi_recv.at[k], to_out)

    def result(k, total):
        j, n = lax.rem(k, UNIT) // PIECES, lax.rem(k, PIECES)
        y[pl.ds(pl.multiple_of(j * rows, rows), rows), pl.ds(pl.multiple_of(n * width, width), width)] = total.astype(BF16)

    def order(k, held, units):
        first = UNIT - held
        rest = units * UNIT - held
        return jnp.where(k < first, k, jnp.where(k < rest, k + held, k - rest + first))

    for b in range(PARTS):
        own_to_in(b).start()

        @pl.when(jnp.logical_not(is_end))
        def _(b=b):
            own_to_out(b).start()

        own_to_sibling(b).start()

    weights[0].wait()
    weights[1].wait()

    @pl.loop(0, CHUNKS)
    def _(j):
        for h in range(HALVES):
            load(j, h, x_part(j * HALVES + h))

        @pl.loop(0, tiles)
        def _(i):
            hidden_tile(j, i)

    weights[2].wait()

    def end_pieces(start, stop):
        @pl.loop(start, stop + AHEAD)
        def _(k):
            @pl.when(k < stop)
            def _():
                piece = order(k, HELD_END, 3)
                term(flow1, k, CHUNKS + piece // PIECES, lax.rem(piece, PIECES))

            @pl.when(k >= start + AHEAD)
            def _():
                piece = order(k - AHEAD, HELD_END, 3)
                rse[piece] = chip_sum(flow1, k - AHEAD).astype(BF16)
                end_sum_in(piece).start()

    @pl.when(is_end)
    def _():
        @pl.loop(0, 3 * CHUNKS)
        def _(a):
            c = CHUNKS + a
            for h in range(HALVES):
                part = a * HALVES + h
                wait_arrival(part)
                on_to_sibling(part).start()
                load(c, h, tm.at[part])
                if h == 0:
                    hidden_first()
                else:
                    hidden_second(c)

            start = a * PIECES - jnp.where(a >= CHUNKS, HELD_END, 0)
            stop = (a + 1) * PIECES - jnp.where(a >= CHUNKS - 1, HELD_END, 0)
            end_pieces(start, stop)

        end_pieces(3 * UNIT - HELD_END, 3 * UNIT)

        @pl.loop(0, UNIT + AHEAD)
        def _(k):
            @pl.when(k < UNIT)
            def _():
                term(flow2, k, k // PIECES, lax.rem(k, PIECES))

            @pl.when(k >= AHEAD)
            def _():
                q = k - AHEAD
                total = chip_sum(flow2, q)
                sum_out(UNIT + q).wait_recv()
                result(q, total + rsi[UNIT + q].astype(F32))

        wait_bytes(rse, 3 * UNIT, rse_send)
        wait_bytes(tm, PARTS, ti_send)

    @pl.when(jnp.logical_not(is_end))
    def _():
        def inner_arrivals(j, h):
            b = j * HALVES + h
            wait_arrival(b)
            on_to_in(b).start()
            on_to_sibling(b).start()
            wait_arrival(PARTS + b)
            on_to_out(PARTS + b).start()
            on_to_sibling(PARTS + b).start()

        def far(j, h):
            a = 2 * PARTS + j * HALVES + h
            wait_arrival(a)
            on_to_out(a).start()
            on_to_sibling(a).start()

        def load_arrived(c, h):
            load(c, h, tm.at[(c - CHUNKS) * HALVES + h])

        @pl.loop(0, CHUNKS)
        def _(j):
            inner_arrivals(j, 0)
            load_arrived(CHUNKS + j, 0)
            hidden_first()
            inner_arrivals(j, 1)
            load_arrived(CHUNKS + j, 1)
            hidden_second(CHUNKS + j)
            load_arrived(2 * CHUNKS + j, 0)
            load_arrived(2 * CHUNKS + j, 1)

            @pl.loop(0, tiles)
            def _(i):
                hidden_tile(2 * CHUNKS + j, i)

        far(0, 0)
        load_arrived(3 * CHUNKS, 0)
        hidden_first()
        far(0, 1)
        load_arrived(3 * CHUNKS, 1)
        hidden_second(3 * CHUNKS)
        last = 4 * CHUNKS - 1

        def term1(k):
            piece = order(k, HELD_INNER, 2)
            term(flow1, k, 2 * CHUNKS + piece // PIECES, lax.rem(piece, PIECES))

        def place2(p):
            first, rest = UNIT - HELD, 2 * UNIT - HELD_INNER
            piece = jnp.where(p < first, p, jnp.where(p < rest, p + HELD_INNER, p - rest + first))
            count = jnp.where(p < first, p, p - (HELD - HELD_INNER))
            return piece, count, jnp.logical_or(p < first, p >= UNIT - HELD_INNER)

        stop2 = 2 * UNIT - HELD_INNER + HELD

        def term2(p):
            piece, count, present = place2(p)

            @pl.when(jnp.logical_and(present, jnp.logical_and(p >= 0, p < stop2)))
            def _():
                term(flow2, count, piece // PIECES, lax.rem(piece, PIECES))

        term1(0)

        @pl.loop(0, stop2 + LAG)
        def _(p):
            @pl.when(p < 2 * UNIT)
            def _():
                k = UNIT + order(p, HELD_INNER, 2)
                total = chip_sum(flow1, p)
                end_sum_in(k).wait_recv()
                rse[k] = (total + rse[k].astype(F32)).astype(BF16)
                inner_sum_in(k).start()

            @pl.when(p < 2 * UNIT - 1)
            def _():
                term1(p + 1)

            q, count, present = place2(p - LAG)

            @pl.when(jnp.logical_and(p >= LAG, present))
            def _():
                total = chip_sum(flow2, count)
                sum_out(q).wait_recv()
                total = total + rsi[q].astype(F32)

                @pl.when(q < UNIT)
                def _():
                    end_sum_in(q).wait_recv()
                    result(q, total + rse[q].astype(F32))

                @pl.when(q >= UNIT)
                def _():
                    rsi[q] = total.astype(BF16)
                    sum_out(q).start()

            term2(p - LAG + 1)

            @pl.when(p == FAR)
            def _():
                far(1, 0)
                far(1, 1)

            @pl.when(p == FAR + 2)
            def _():
                load_arrived(last, 0)
                load_arrived(last, 1)

            @pl.when(jnp.logical_and(p >= FAR + 2, p < FAR + 2 + tiles))
            def _():
                hidden_tile(last, p - FAR - 2)

        wait_bytes(rse, 2 * UNIT, rse_send)
        wait_bytes(rsi, UNIT, rsi_send)
        wait_bytes(tm, 2 * PARTS, ti_send)
        wait_bytes(tm, 3 * PARTS, te_send)

    drain(flow1)
    drain(flow2)
    wait_bytes(ts, 4 * PARTS, ts_send)


def solution(mesh):
    def step(x, w_gate, w_up, w_down):
        n_rows, d = x.shape
        ff = w_gate.shape[1]
        rows, width = n_rows // CHUNKS, d // PIECES
        dma = pltpu.SemaphoreType.DMA
        out, _, _ = pl.pallas_call(
            kernel,
            out_shape=[
                pltpu.VMEM((n_rows, d), BF16),
                jax.ShapeDtypeStruct((3 * PARTS, rows, d // HALVES), BF16),
                jax.ShapeDtypeStruct((4 * PARTS, rows, d // HALVES), BF16),
            ],
            in_specs=[pl.BlockSpec(memory_space=pltpu.HBM)] * 4,
            out_specs=[pl.BlockSpec(memory_space=pltpu.VMEM)] + [pl.BlockSpec(memory_space=pltpu.HBM)] * 2,
            scratch_shapes=[
                pltpu.VMEM((d, ff), BF16),
                pltpu.VMEM((d, ff), BF16),
                pltpu.VMEM((ff, d), BF16),
                pltpu.VMEM((HALVES, 2 * rows, d // HALVES), BF16),
                pltpu.VMEM((2, 2 * rows, ff), F32),
                pltpu.VMEM((4 * CHUNKS, 2 * rows, ff), BF16),
                *[
                    pltpu.VMEM((RING, rows, width), F32),
                    pltpu.VMEM((RING, rows, width), BF16),
                    pltpu.VMEM((RING, rows, width), BF16),
                ]
                * 2,
                pltpu.VMEM((3 * UNIT, rows, width), BF16),
                pltpu.VMEM((2 * UNIT, rows, width), BF16),
                dma((3,)),
                dma((2,)),
                dma((3 * PARTS,)),
                dma((4 * PARTS,)),
                dma,
                dma,
                dma,
                dma((RING,)),
                dma((RING,)),
                dma((RING,)),
                dma((RING,)),
                dma,
                dma((3 * UNIT,)),
                dma,
                dma((2 * UNIT,)),
            ],
            compiler_params=pltpu.CompilerParams(
                collective_id=0, has_side_effects=True, vmem_limit_bytes=64_000_000
            ),
            name="mlp_line",
        )(x, w_gate, w_up, w_down)
        return out

    return jax.shard_map(
        step,
        mesh=mesh,
        in_specs=(P(("dp", "tp"), None), P(None, "tp"), P(None, "tp"), P("tp", None)),
        out_specs=P(("dp", "tp"), None),
        check_vma=False,
    )
```

```python
import functools

import jax
import jax.numpy as jnp
from jax import lax
from jax.experimental import pallas as pl
from jax.experimental.pallas import tpu as pltpu
from jax.sharding import PartitionSpec as P

MESH = pl.DeviceIdType.MESH
F32, BF16 = jnp.float32, jnp.bfloat16

CHUNKS = 2
HALVES = 2
PARTS = CHUNKS * HALVES
PIECES = 8
RING = 6
AHEAD = 2
NEXT = 2
LAG = 2
HELD_END, HELD_INNER = 4, 2
UNIT = CHUNKS * PIECES
HELD = max(HELD_END, HELD_INNER)
EARLY = UNIT - HELD
FAR = 3


def kernel(
    x, wg, wu, wd, y, tm, ts, vwg, vwu, vwd, xb, acc, hid,
    own1, sib1, stg1, own2, sib2, stg2, rse, rsi,
    w_sem, x_sem, tm_recv, ts_recv, ti_send, te_send, ts_send,
    d1_send, d1_recv, d2_send, d2_recv, rse_send, rse_recv, rsi_send, rsi_recv,
):
    me = lax.axis_index("tp")
    chip, core = me // 2, lax.rem(me, 2)
    is_end = jnp.logical_or(chip == 0, chip == 3)
    sibling = me + 1 - 2 * core
    inward = jnp.where(chip < 2, 2, -2)
    to_in, to_out = me + inward, me - inward
    rows, half = x.shape[0] // CHUNKS, x.shape[1] // HALVES
    width = y.shape[1] // PIECES
    tile = min(256, vwg.shape[1])
    tiles = vwg.shape[1] // tile

    barrier = pltpu.get_barrier_semaphore()
    pl.semaphore_signal(barrier, inc=1, device_id={"tp": sibling}, device_id_type=MESH)
    pl.semaphore_signal(barrier, inc=1, device_id={"tp": to_in}, device_id_type=MESH)

    @pl.when(jnp.logical_not(is_end))
    def _():
        pl.semaphore_signal(barrier, inc=1, device_id={"tp": to_out}, device_id_type=MESH)

    weights = [pltpu.make_async_copy(s, d, w_sem.at[i]) for i, (s, d) in enumerate(((wg, vwg), (wu, vwu), (wd, vwd)))]
    for w in weights:
        w.start()

    pl.semaphore_wait(barrier, jnp.where(is_end, 2, 3))

    def remote(src, dst, send, recv, device):
        return pltpu.make_async_remote_copy(
            src_ref=src, dst_ref=dst, send_sem=send, recv_sem=recv, device_id={"tp": device}, device_id_type=MESH
        )

    def x_part(b):
        j, h = b // HALVES, lax.rem(b, HALVES)
        return x.at[pl.ds(pl.multiple_of(j * rows, rows), rows), pl.ds(pl.multiple_of(h * half, half), half)]

    def own_to_in(b):
        slot = jnp.where(is_end, 0, PARTS) + b
        return remote(x_part(b), tm.at[slot], ti_send, tm_recv.at[slot], to_in)

    def own_to_out(b):
        return remote(x_part(b), tm.at[b], te_send, tm_recv.at[b], to_out)

    def own_to_sibling(b):
        return remote(x_part(b), ts.at[b], ts_send, ts_recv.at[0], sibling)

    def on_to_in(b):
        slot = 2 * PARTS + b
        return remote(tm.at[b], tm.at[slot], ti_send, tm_recv.at[slot], to_in)

    def on_to_out(a):
        return remote(tm.at[a], tm.at[a], te_send, tm_recv.at[a], to_out)

    def on_to_sibling(a):
        return remote(tm.at[a], ts.at[PARTS + a], ts_send, ts_recv.at[1 + a], sibling)

    def wait_arrival(a):
        on_to_out(a).wait_recv()

    def wait_bytes(ref, count, sem):
        whole = ref.at[pl.ds(0, count)]
        pltpu.make_async_copy(whole, whole, sem).wait()

    def load(c, h, mine):
        theirs = ts.at[c * HALVES + h]
        first = pltpu.make_async_copy(mine, xb.at[h, pl.ds(0, rows)], x_sem.at[0])
        second = pltpu.make_async_copy(theirs, xb.at[h, pl.ds(rows, rows)], x_sem.at[1])
        first.start()
        second.start()
        first.wait()
        second.wait()

    def load_arrived(c, h):
        part = (c - CHUNKS) * HALVES + h
        on_to_sibling(part).wait_recv()
        load(c, h, tm.at[part])

    def product(weight, columns, h):
        return jnp.dot(xb[h], weight[pl.ds(h * half, half), columns], preferred_element_type=F32)

    def finish(c, columns, gate, up):
        hid[c, :, columns] = (jax.nn.gelu(gate) * up).astype(BF16)

    def hidden_tile(c, i):
        columns = pl.ds(pl.multiple_of(i * tile, tile), tile)
        gate = product(vwg, columns, 0) + product(vwg, columns, 1)
        up = product(vwu, columns, 0) + product(vwu, columns, 1)
        finish(c, columns, gate, up)

    def hidden_first():
        @pl.loop(0, tiles)
        def _(i):
            columns = pl.ds(pl.multiple_of(i * tile, tile), tile)
            acc[0, :, columns] = product(vwg, columns, 0)
            acc[1, :, columns] = product(vwu, columns, 0)

    def hidden_second(c):
        @pl.loop(0, tiles)
        def _(i):
            columns = pl.ds(pl.multiple_of(i * tile, tile), tile)
            gate = acc[0, :, columns] + product(vwg, columns, 1)
            up = acc[1, :, columns] + product(vwu, columns, 1)
            finish(c, columns, gate, up)

    def to_sibling(stg, sib, send, recv, k):
        s = lax.rem(k, RING)
        return remote(stg.at[s], sib.at[s], send.at[s], recv.at[s], sibling)

    def term(flow, k, c, n):
        own, sib, stg, send, recv = flow
        s = lax.rem(k, RING)

        @pl.when(k >= RING)
        def _():
            to_sibling(stg, sib, send, recv, k).wait_send()

        columns = pl.ds(pl.multiple_of(n * width, width), width)
        both = jnp.dot(hid[c], vwd[:, columns], preferred_element_type=F32)
        stg[s] = both[rows:].astype(BF16)
        own[s] = both[:rows]
        to_sibling(stg, sib, send, recv, k).start()

    def chip_sum(flow, k):
        own, sib, stg, send, recv = flow
        s = lax.rem(k, RING)
        to_sibling(stg, sib, send, recv, k).wait_recv()
        return own[s] + sib[s].astype(F32)

    def drain(flow):
        own, sib, stg, send, recv = flow

        @pl.loop(0, RING)
        def _(k):
            to_sibling(stg, sib, send, recv, k).wait_send()

    flow1 = (own1, sib1, stg1, d1_send, d1_recv)
    flow2 = (own2, sib2, stg2, d2_send, d2_recv)

    def end_sum_in(k):
        return remote(rse.at[k], rse.at[k], rse_send, rse_recv.at[jnp.maximum(k - EARLY + 1, 0)], to_in)

    def inner_sum_in(k):
        return remote(rse.at[k], rsi.at[k - UNIT], rse_send, rsi_recv.at[k - UNIT], to_in)

    def sum_out(k):
        return remote(rsi.at[k], rsi.at[k], rsi_send, rsi_recv.at[k], to_out)

    def result(k, total):
        j, n = lax.rem(k, UNIT) // PIECES, lax.rem(k, PIECES)
        y[pl.ds(pl.multiple_of(j * rows, rows), rows), pl.ds(pl.multiple_of(n * width, width), width)] = total.astype(BF16)

    def order(k, held, units):
        first = UNIT - held
        rest = units * UNIT - held
        return jnp.where(k < first, k, jnp.where(k < rest, k + held, k - rest + first))

    for b in range(PARTS):
        own_to_in(b).start()

        @pl.when(jnp.logical_not(is_end))
        def _(b=b):
            own_to_out(b).start()

        own_to_sibling(b).start()

    weights[0].wait()
    weights[1].wait()

    wait_bytes(ts, PARTS, ts_recv.at[0])

    @pl.loop(0, CHUNKS)
    def _(j):
        for h in range(HALVES):
            load(j, h, x_part(j * HALVES + h))

        @pl.loop(0, tiles)
        def _(i):
            hidden_tile(j, i)

    weights[2].wait()

    def end_pieces(start, stop):
        @pl.loop(start, stop + AHEAD)
        def _(k):
            @pl.when(k < stop)
            def _():
                piece = order(k, HELD_END, 3)
                term(flow1, k, CHUNKS + piece // PIECES, lax.rem(piece, PIECES))

            @pl.when(k >= start + AHEAD)
            def _():
                piece = order(k - AHEAD, HELD_END, 3)
                rse[piece] = chip_sum(flow1, k - AHEAD).astype(BF16)
                end_sum_in(piece).start()

    @pl.when(is_end)
    def _():
        @pl.loop(0, 3 * CHUNKS)
        def _(a):
            c = CHUNKS + a
            for h in range(HALVES):
                part = a * HALVES + h
                wait_arrival(part)
                on_to_sibling(part).start()
                load_arrived(c, h)
                if h == 0:
                    hidden_first()
                else:
                    hidden_second(c)

            start = a * PIECES - jnp.where(a >= CHUNKS, HELD_END, 0)
            stop = (a + 1) * PIECES - jnp.where(a >= CHUNKS - 1, HELD_END, 0)
            end_pieces(start, stop)

        end_pieces(3 * UNIT - HELD_END, 3 * UNIT)

        @pl.loop(0, UNIT + AHEAD)
        def _(k):
            @pl.when(k < UNIT)
            def _():
                term(flow2, k, k // PIECES, lax.rem(k, PIECES))

            @pl.when(k >= AHEAD)
            def _():
                q = k - AHEAD
                total = chip_sum(flow2, q)
                sum_out(UNIT + q).wait_recv()
                result(q, total + rsi[UNIT + q].astype(F32))

        wait_bytes(rse, 3 * UNIT, rse_send)
        wait_bytes(tm, PARTS, ti_send)

    @pl.when(jnp.logical_not(is_end))
    def _():
        def inner_arrivals(j, h):
            b = j * HALVES + h
            wait_arrival(b)
            on_to_in(b).start()
            on_to_sibling(b).start()
            wait_arrival(PARTS + b)
            on_to_out(PARTS + b).start()
            on_to_sibling(PARTS + b).start()

        def far(j, h):
            a = 2 * PARTS + j * HALVES + h
            wait_arrival(a)
            on_to_out(a).start()
            on_to_sibling(a).start()

        @pl.loop(0, CHUNKS)
        def _(j):
            inner_arrivals(j, 0)
            load_arrived(CHUNKS + j, 0)
            hidden_first()
            inner_arrivals(j, 1)
            load_arrived(CHUNKS + j, 1)
            hidden_second(CHUNKS + j)
            load_arrived(2 * CHUNKS + j, 0)
            load_arrived(2 * CHUNKS + j, 1)

            @pl.loop(0, tiles)
            def _(i):
                hidden_tile(2 * CHUNKS + j, i)

        far(0, 0)
        load_arrived(3 * CHUNKS, 0)
        hidden_first()
        far(0, 1)
        load_arrived(3 * CHUNKS, 1)
        hidden_second(3 * CHUNKS)
        last = 4 * CHUNKS - 1

        def term1(k):
            piece = order(k, HELD_INNER, 2)
            term(flow1, k, 2 * CHUNKS + piece // PIECES, lax.rem(piece, PIECES))

        def place2(p):
            first, rest = UNIT - HELD, 2 * UNIT - HELD_INNER
            piece = jnp.where(p < first, p, jnp.where(p < rest, p + HELD_INNER, p - rest + first))
            count = jnp.where(p < first, p, p - (HELD - HELD_INNER))
            return piece, count, jnp.logical_or(p < first, p >= UNIT - HELD_INNER)

        stop2 = 2 * UNIT - HELD_INNER + HELD

        def term2(p):
            piece, count, present = place2(p)

            @pl.when(jnp.logical_and(present, jnp.logical_and(p >= 0, p < stop2)))
            def _():
                term(flow2, count, piece // PIECES, lax.rem(piece, PIECES))

        for k in range(NEXT):
            term1(k)

        for k in range(NEXT - LAG):
            term2(k)

        @pl.loop(0, stop2 + LAG)
        def _(p):
            @pl.when(p < 2 * UNIT)
            def _():
                k = UNIT + order(p, HELD_INNER, 2)
                total = chip_sum(flow1, p)
                end_sum_in(k).wait_recv()
                rse[k] = (total + rse[k].astype(F32)).astype(BF16)
                inner_sum_in(k).start()

            @pl.when(p < 2 * UNIT - NEXT)
            def _():
                term1(p + NEXT)

            q, count, present = place2(p - LAG)

            @pl.when(jnp.logical_and(p >= LAG, present))
            def _():
                total = chip_sum(flow2, count)
                sum_out(q).wait_recv()
                total = total + rsi[q].astype(F32)

                @pl.when(q == 0)
                def _():
                    wait_bytes(rse, EARLY, rse_recv.at[0])

                @pl.when(jnp.logical_and(q >= EARLY, q < UNIT))
                def _():
                    end_sum_in(q).wait_recv()

                @pl.when(q < UNIT)
                def _():
                    result(q, total + rse[q].astype(F32))

                @pl.when(q >= UNIT)
                def _():
                    rsi[q] = total.astype(BF16)
                    sum_out(q).start()

            term2(p - LAG + NEXT)

            @pl.when(p == FAR)
            def _():
                far(1, 0)
                far(1, 1)

            @pl.when(p == FAR + 2)
            def _():
                load_arrived(last, 0)
                load_arrived(last, 1)

            @pl.when(jnp.logical_and(p >= FAR + 2, p < FAR + 2 + tiles))
            def _():
                hidden_tile(last, p - FAR - 2)

        wait_bytes(rse, 2 * UNIT, rse_send)
        wait_bytes(rsi, UNIT, rsi_send)
        wait_bytes(tm, 2 * PARTS, ti_send)
        wait_bytes(tm, 3 * PARTS, te_send)

    drain(flow1)
    drain(flow2)
    wait_bytes(ts, 4 * PARTS, ts_send)


def solution(mesh):
    def step(x, w_gate, w_up, w_down):
        n_rows, d = x.shape
        ff = w_gate.shape[1]
        rows, width = n_rows // CHUNKS, d // PIECES
        dma = pltpu.SemaphoreType.DMA
        out, _, _ = pl.pallas_call(
            kernel,
            out_shape=[
                pltpu.VMEM((n_rows, d), BF16),
                jax.ShapeDtypeStruct((3 * PARTS, rows, d // HALVES), BF16),
                jax.ShapeDtypeStruct((4 * PARTS, rows, d // HALVES), BF16),
            ],
            in_specs=[pl.BlockSpec(memory_space=pltpu.HBM)] * 4,
            out_specs=[pl.BlockSpec(memory_space=pltpu.VMEM)] + [pl.BlockSpec(memory_space=pltpu.HBM)] * 2,
            scratch_shapes=[
                pltpu.VMEM((d, ff), BF16),
                pltpu.VMEM((d, ff), BF16),
                pltpu.VMEM((ff, d), BF16),
                pltpu.VMEM((HALVES, 2 * rows, d // HALVES), BF16),
                pltpu.VMEM((2, 2 * rows, ff), F32),
                pltpu.VMEM((4 * CHUNKS, 2 * rows, ff), BF16),
                *[
                    pltpu.VMEM((RING, rows, width), F32),
                    pltpu.VMEM((RING, rows, width), BF16),
                    pltpu.VMEM((RING, rows, width), BF16),
                ]
                * 2,
                pltpu.VMEM((3 * UNIT, rows, width), BF16),
                pltpu.VMEM((2 * UNIT, rows, width), BF16),
                dma((3,)),
                dma((2,)),
                dma((3 * PARTS,)),
                dma((3 * PARTS + 1,)),
                dma,
                dma,
                dma,
                dma((RING,)),
                dma((RING,)),
                dma((RING,)),
                dma((RING,)),
                dma,
                dma((3 * UNIT - EARLY + 1,)),
                dma,
                dma((2 * UNIT,)),
            ],
            compiler_params=pltpu.CompilerParams(
                collective_id=0, has_side_effects=True, vmem_limit_bytes=64_000_000
            ),
            name="mlp_line",
        )(x, w_gate, w_up, w_down)
        return out

    return jax.shard_map(
        step,
        mesh=mesh,
        in_specs=(P(("dp", "tp"), None), P(None, "tp"), P(None, "tp"), P("tp", None)),
        out_specs=P(("dp", "tp"), None),
        check_vma=False,
    )
```

```python
import functools

import jax
import jax.numpy as jnp
from jax import lax
from jax.experimental import pallas as pl
from jax.experimental.pallas import tpu as pltpu
from jax.sharding import PartitionSpec as P

MESH = pl.DeviceIdType.MESH
F32, BF16 = jnp.float32, jnp.bfloat16

CHUNKS = 2
HALVES = 2
PARTS = CHUNKS * HALVES
PIECES = 8
RING = 6
AHEAD = 2
NEXT = 2
LAG = 2
HELD_END, HELD_INNER = 4, 2
UNIT = CHUNKS * PIECES
HELD = max(HELD_END, HELD_INNER)
EARLY = UNIT - HELD
FAR = 3


def kernel(
    x, wg, wu, wd, y, tm, ts, vwg, vwu, vwd, xb, acc, hid,
    own1, sib1, stg1, own2, sib2, stg2, rse, rsi,
    ready, w_sem, x_sem, tm_recv, ts_recv, ti_send, te_send, ts_send,
    d1_send, d1_recv, d2_send, d2_recv, rse_send, rse_recv, rsi_send, rsi_recv,
):
    me = lax.axis_index("tp")
    chip, core = me // 2, lax.rem(me, 2)
    is_end = jnp.logical_or(chip == 0, chip == 3)
    sibling = me + 1 - 2 * core
    inward = jnp.where(chip < 2, 2, -2)
    to_in, to_out = me + inward, me - inward
    rows, half = x.shape[0] // CHUNKS, x.shape[1] // HALVES
    width = y.shape[1] // PIECES
    tile = min(256, vwg.shape[1])
    tiles = vwg.shape[1] // tile

    barrier = pltpu.get_barrier_semaphore()
    def signal(semaphore, device):
        pl.semaphore_signal(semaphore, inc=1, device_id={"tp": device}, device_id_type=MESH)

    signal(barrier, sibling)

    @pl.when(is_end)
    def _():
        signal(barrier, to_in - core)

    @pl.when(jnp.logical_not(is_end))
    def _():
        signal(barrier, to_out)
        signal(barrier, to_in - core + 1)

    weights = [pltpu.make_async_copy(s, d, w_sem.at[i]) for i, (s, d) in enumerate(((wg, vwg), (wu, vwu), (wd, vwd)))]
    for w in weights:
        w.start()

    pl.semaphore_wait(barrier, jnp.where(is_end, 2, 3))

    def remote(src, dst, send, recv, device):
        return pltpu.make_async_remote_copy(
            src_ref=src, dst_ref=dst, send_sem=send, recv_sem=recv, device_id={"tp": device}, device_id_type=MESH
        )

    def x_part(b):
        j, h = b // HALVES, lax.rem(b, HALVES)
        return x.at[pl.ds(pl.multiple_of(j * rows, rows), rows), pl.ds(pl.multiple_of(h * half, half), half)]

    def own_to_in(b):
        slot = jnp.where(is_end, 0, PARTS) + b
        return remote(x_part(b), tm.at[slot], ti_send, tm_recv.at[slot], to_in)

    def own_to_out(b):
        return remote(x_part(b), tm.at[b], te_send, tm_recv.at[b], to_out)

    def own_to_sibling(b):
        return remote(x_part(b), ts.at[b], ts_send, ts_recv.at[0], sibling)

    def on_to_in(b):
        slot = 2 * PARTS + b
        return remote(tm.at[b], tm.at[slot], ti_send, tm_recv.at[slot], to_in)

    def on_to_out(a):
        return remote(tm.at[a], tm.at[a], te_send, tm_recv.at[a], to_out)

    def on_to_sibling(a):
        return remote(tm.at[a], ts.at[PARTS + a], ts_send, ts_recv.at[1 + a], sibling)

    def wait_arrival(a):
        on_to_out(a).wait_recv()

    def wait_bytes(ref, count, sem):
        whole = ref.at[pl.ds(0, count)]
        pltpu.make_async_copy(whole, whole, sem).wait()

    def load(c, h, mine):
        theirs = ts.at[c * HALVES + h]
        first = pltpu.make_async_copy(mine, xb.at[h, pl.ds(0, rows)], x_sem.at[0])
        second = pltpu.make_async_copy(theirs, xb.at[h, pl.ds(rows, rows)], x_sem.at[1])
        first.start()
        second.start()
        first.wait()
        second.wait()

    def load_arrived(c, h):
        part = (c - CHUNKS) * HALVES + h
        on_to_sibling(part).wait_recv()
        load(c, h, tm.at[part])

    def product(weight, columns, h):
        return jnp.dot(xb[h], weight[pl.ds(h * half, half), columns], preferred_element_type=F32)

    def finish(c, columns, gate, up):
        hid[c, :, columns] = (jax.nn.gelu(gate) * up).astype(BF16)

    def hidden_tile(c, i):
        columns = pl.ds(pl.multiple_of(i * tile, tile), tile)
        gate = product(vwg, columns, 0) + product(vwg, columns, 1)
        up = product(vwu, columns, 0) + product(vwu, columns, 1)
        finish(c, columns, gate, up)

    def hidden_first():
        @pl.loop(0, tiles)
        def _(i):
            columns = pl.ds(pl.multiple_of(i * tile, tile), tile)
            acc[0, :, columns] = product(vwg, columns, 0)
            acc[1, :, columns] = product(vwu, columns, 0)

    def hidden_second(c):
        @pl.loop(0, tiles)
        def _(i):
            columns = pl.ds(pl.multiple_of(i * tile, tile), tile)
            gate = acc[0, :, columns] + product(vwg, columns, 1)
            up = acc[1, :, columns] + product(vwu, columns, 1)
            finish(c, columns, gate, up)

    def to_sibling(stg, sib, send, recv, k):
        s = lax.rem(k, RING)
        return remote(stg.at[s], sib.at[s], send.at[s], recv.at[s], sibling)

    def term(flow, k, c, n):
        own, sib, stg, send, recv = flow
        s = lax.rem(k, RING)

        @pl.when(k >= RING)
        def _():
            to_sibling(stg, sib, send, recv, k).wait_send()

        columns = pl.ds(pl.multiple_of(n * width, width), width)
        both = jnp.dot(hid[c], vwd[:, columns], preferred_element_type=F32)
        stg[s] = both[rows:].astype(BF16)
        own[s] = both[:rows]
        to_sibling(stg, sib, send, recv, k).start()

    def chip_sum(flow, k):
        own, sib, stg, send, recv = flow
        s = lax.rem(k, RING)
        to_sibling(stg, sib, send, recv, k).wait_recv()
        return own[s] + sib[s].astype(F32)

    def drain(flow):
        own, sib, stg, send, recv = flow

        @pl.loop(0, RING)
        def _(k):
            to_sibling(stg, sib, send, recv, k).wait_send()

    flow1 = (own1, sib1, stg1, d1_send, d1_recv)
    flow2 = (own2, sib2, stg2, d2_send, d2_recv)

    def end_sum_in(k):
        return remote(rse.at[k], rse.at[k], rse_send, rse_recv.at[jnp.maximum(k - EARLY + 1, 0)], to_in)

    def inner_sum_in(k):
        return remote(rse.at[k], rsi.at[k - UNIT], rse_send, rsi_recv.at[k - UNIT], to_in)

    def sum_out(k):
        return remote(rsi.at[k], rsi.at[k], rsi_send, rsi_recv.at[k], to_out)

    def result(k, total):
        j, n = lax.rem(k, UNIT) // PIECES, lax.rem(k, PIECES)
        y[pl.ds(pl.multiple_of(j * rows, rows), rows), pl.ds(pl.multiple_of(n * width, width), width)] = total.astype(BF16)

    def order(k, held, units):
        first = UNIT - held
        rest = units * UNIT - held
        return jnp.where(k < first, k, jnp.where(k < rest, k + held, k - rest + first))

    def all_parts(copy):
        for b in range(PARTS):
            copy(b).start()

    is_inner = jnp.logical_not(is_end)

    @pl.when(jnp.logical_or(is_end, core == 1))
    def _():
        all_parts(own_to_in)

    @pl.when(jnp.logical_and(is_inner, core == 0))
    def _():
        all_parts(own_to_out)

    @pl.when(is_inner)
    def _():
        signal(ready, sibling)

    all_parts(own_to_sibling)

    @pl.when(is_inner)
    def _():
        pl.semaphore_wait(ready, 1)

    @pl.when(jnp.logical_and(is_inner, core == 0))
    def _():
        all_parts(own_to_in)

    @pl.when(jnp.logical_and(is_inner, core == 1))
    def _():
        all_parts(own_to_out)

    weights[0].wait()
    weights[1].wait()

    wait_bytes(ts, PARTS, ts_recv.at[0])

    @pl.loop(0, CHUNKS)
    def _(j):
        for h in range(HALVES):
            load(j, h, x_part(j * HALVES + h))

        @pl.loop(0, tiles)
        def _(i):
            hidden_tile(j, i)

    weights[2].wait()

    def end_pieces(start, stop):
        @pl.loop(start, stop + AHEAD)
        def _(k):
            @pl.when(k < stop)
            def _():
                piece = order(k, HELD_END, 3)
                term(flow1, k, CHUNKS + piece // PIECES, lax.rem(piece, PIECES))

            @pl.when(k >= start + AHEAD)
            def _():
                piece = order(k - AHEAD, HELD_END, 3)
                rse[piece] = chip_sum(flow1, k - AHEAD).astype(BF16)
                end_sum_in(piece).start()

    @pl.when(is_end)
    def _():
        @pl.loop(0, 3 * CHUNKS)
        def _(a):
            c = CHUNKS + a
            for h in range(HALVES):
                part = a * HALVES + h
                wait_arrival(part)
                on_to_sibling(part).start()
                load_arrived(c, h)
                if h == 0:
                    hidden_first()
                else:
                    hidden_second(c)

            start = a * PIECES - jnp.where(a >= CHUNKS, HELD_END, 0)
            stop = (a + 1) * PIECES - jnp.where(a >= CHUNKS - 1, HELD_END, 0)
            end_pieces(start, stop)

        end_pieces(3 * UNIT - HELD_END, 3 * UNIT)

        @pl.loop(0, UNIT + AHEAD)
        def _(k):
            @pl.when(k < UNIT)
            def _():
                term(flow2, k, k // PIECES, lax.rem(k, PIECES))

            @pl.when(k >= AHEAD)
            def _():
                q = k - AHEAD
                total = chip_sum(flow2, q)
                sum_out(UNIT + q).wait_recv()
                result(q, total + rsi[UNIT + q].astype(F32))

        wait_bytes(rse, 3 * UNIT, rse_send)
        wait_bytes(tm, PARTS, ti_send)

    @pl.when(jnp.logical_not(is_end))
    def _():
        def inner_arrivals(j, h):
            b = j * HALVES + h
            wait_arrival(b)
            on_to_in(b).start()
            on_to_sibling(b).start()
            wait_arrival(PARTS + b)
            on_to_out(PARTS + b).start()
            on_to_sibling(PARTS + b).start()

        def far(j, h):
            a = 2 * PARTS + j * HALVES + h
            wait_arrival(a)
            on_to_out(a).start()
            on_to_sibling(a).start()

        @pl.loop(0, CHUNKS)
        def _(j):
            inner_arrivals(j, 0)
            load_arrived(CHUNKS + j, 0)
            hidden_first()
            inner_arrivals(j, 1)
            load_arrived(CHUNKS + j, 1)
            hidden_second(CHUNKS + j)
            load_arrived(2 * CHUNKS + j, 0)
            load_arrived(2 * CHUNKS + j, 1)

            @pl.loop(0, tiles)
            def _(i):
                hidden_tile(2 * CHUNKS + j, i)

        far(0, 0)
        load_arrived(3 * CHUNKS, 0)
        hidden_first()
        far(0, 1)
        load_arrived(3 * CHUNKS, 1)
        hidden_second(3 * CHUNKS)
        last = 4 * CHUNKS - 1

        def term1(k):
            piece = order(k, HELD_INNER, 2)
            term(flow1, k, 2 * CHUNKS + piece // PIECES, lax.rem(piece, PIECES))

        def place2(p):
            first, rest = UNIT - HELD, 2 * UNIT - HELD_INNER
            piece = jnp.where(p < first, p, jnp.where(p < rest, p + HELD_INNER, p - rest + first))
            count = jnp.where(p < first, p, p - (HELD - HELD_INNER))
            return piece, count, jnp.logical_or(p < first, p >= UNIT - HELD_INNER)

        stop2 = 2 * UNIT - HELD_INNER + HELD

        def term2(p):
            piece, count, present = place2(p)

            @pl.when(jnp.logical_and(present, jnp.logical_and(p >= 0, p < stop2)))
            def _():
                term(flow2, count, piece // PIECES, lax.rem(piece, PIECES))

        for k in range(NEXT):
            term1(k)

        for k in range(NEXT - LAG):
            term2(k)

        @pl.loop(0, stop2 + LAG)
        def _(p):
            @pl.when(p < 2 * UNIT)
            def _():
                k = UNIT + order(p, HELD_INNER, 2)
                total = chip_sum(flow1, p)
                end_sum_in(k).wait_recv()
                rse[k] = (total + rse[k].astype(F32)).astype(BF16)
                inner_sum_in(k).start()

            @pl.when(p < 2 * UNIT - NEXT)
            def _():
                term1(p + NEXT)

            q, count, present = place2(p - LAG)

            @pl.when(jnp.logical_and(p >= LAG, present))
            def _():
                total = chip_sum(flow2, count)
                sum_out(q).wait_recv()
                total = total + rsi[q].astype(F32)

                @pl.when(q == 0)
                def _():
                    wait_bytes(rse, EARLY, rse_recv.at[0])

                @pl.when(jnp.logical_and(q >= EARLY, q < UNIT))
                def _():
                    end_sum_in(q).wait_recv()

                @pl.when(q < UNIT)
                def _():
                    result(q, total + rse[q].astype(F32))

                @pl.when(q >= UNIT)
                def _():
                    rsi[q] = total.astype(BF16)
                    sum_out(q).start()

            term2(p - LAG + NEXT)

            @pl.when(p == FAR)
            def _():
                far(1, 0)
                far(1, 1)

            @pl.when(p == FAR + 2)
            def _():
                load_arrived(last, 0)
                load_arrived(last, 1)

            @pl.when(jnp.logical_and(p >= FAR + 2, p < FAR + 2 + tiles))
            def _():
                hidden_tile(last, p - FAR - 2)

        wait_bytes(rse, 2 * UNIT, rse_send)
        wait_bytes(rsi, UNIT, rsi_send)
        wait_bytes(tm, 2 * PARTS, ti_send)
        wait_bytes(tm, 3 * PARTS, te_send)

    drain(flow1)
    drain(flow2)
    wait_bytes(ts, 4 * PARTS, ts_send)


def solution(mesh):
    def step(x, w_gate, w_up, w_down):
        n_rows, d = x.shape
        ff = w_gate.shape[1]
        rows, width = n_rows // CHUNKS, d // PIECES
        dma = pltpu.SemaphoreType.DMA
        out, _, _ = pl.pallas_call(
            kernel,
            out_shape=[
                pltpu.VMEM((n_rows, d), BF16),
                jax.ShapeDtypeStruct((3 * PARTS, rows, d // HALVES), BF16),
                jax.ShapeDtypeStruct((4 * PARTS, rows, d // HALVES), BF16),
            ],
            in_specs=[pl.BlockSpec(memory_space=pltpu.HBM)] * 4,
            out_specs=[pl.BlockSpec(memory_space=pltpu.VMEM)] + [pl.BlockSpec(memory_space=pltpu.HBM)] * 2,
            scratch_shapes=[
                pltpu.VMEM((d, ff), BF16),
                pltpu.VMEM((d, ff), BF16),
                pltpu.VMEM((ff, d), BF16),
                pltpu.VMEM((HALVES, 2 * rows, d // HALVES), BF16),
                pltpu.VMEM((2, 2 * rows, ff), F32),
                pltpu.VMEM((4 * CHUNKS, 2 * rows, ff), BF16),
                *[
                    pltpu.VMEM((RING, rows, width), F32),
                    pltpu.VMEM((RING, rows, width), BF16),
                    pltpu.VMEM((RING, rows, width), BF16),
                ]
                * 2,
                pltpu.VMEM((3 * UNIT, rows, width), BF16),
                pltpu.VMEM((2 * UNIT, rows, width), BF16),
                pltpu.SemaphoreType.REGULAR,
                dma((3,)),
                dma((2,)),
                dma((3 * PARTS,)),
                dma((3 * PARTS + 1,)),
                dma,
                dma,
                dma,
                dma((RING,)),
                dma((RING,)),
                dma((RING,)),
                dma((RING,)),
                dma,
                dma((3 * UNIT - EARLY + 1,)),
                dma,
                dma((2 * UNIT,)),
            ],
            compiler_params=pltpu.CompilerParams(
                collective_id=0, has_side_effects=True, vmem_limit_bytes=64_000_000
            ),
            name="mlp_line",
        )(x, w_gate, w_up, w_down)
        return out

    return jax.shard_map(
        step,
        mesh=mesh,
        in_specs=(P(("dp", "tp"), None), P(None, "tp"), P(None, "tp"), P("tp", None)),
        out_specs=P(("dp", "tp"), None),
        check_vma=False,
    )
```

```python
import functools

import jax
import jax.numpy as jnp
from jax import lax
from jax.experimental import pallas as pl
from jax.experimental.pallas import tpu as pltpu
from jax.sharding import PartitionSpec as P

MESH = pl.DeviceIdType.MESH
F32, BF16 = jnp.float32, jnp.bfloat16

CHUNKS = 2
HALVES = 2
PARTS = CHUNKS * HALVES
PIECES = 8
RING = 4
AHEAD = 1
NEXT = 2
LAG = 2
HELD_END, HELD_INNER = 4, 2
UNIT = CHUNKS * PIECES
HELD = max(HELD_END, HELD_INNER)
EARLY = UNIT - HELD
FAR = 3


def kernel(
    x, wg, wu, wd, y, tm, ts, vwg, vwu, vwd, xb, acc, hid,
    own1, sib1, stg1, own2, sib2, stg2, rse, rsi,
    ready, free, w_sem, x_sem, tm_recv, ts_recv, ti_send, te_send, ts_send,
    d1_send, d1_recv, d2_send, d2_recv, rse_send, rse_recv, rsi_send, rsi_recv,
):
    me = lax.axis_index("tp")
    chip, core = me // 2, lax.rem(me, 2)
    is_end = jnp.logical_or(chip == 0, chip == 3)
    sibling = me + 1 - 2 * core
    inward = jnp.where(chip < 2, 2, -2)
    to_in, to_out = me + inward, me - inward
    rows, half = x.shape[0] // CHUNKS, x.shape[1] // HALVES
    width = y.shape[1] // PIECES
    tile = min(256, vwg.shape[1])
    tiles = vwg.shape[1] // tile

    barrier = pltpu.get_barrier_semaphore()
    def signal(semaphore, device):
        pl.semaphore_signal(semaphore, inc=1, device_id={"tp": device}, device_id_type=MESH)

    signal(barrier, sibling)

    @pl.when(is_end)
    def _():
        signal(barrier, to_in - core)

    @pl.when(jnp.logical_not(is_end))
    def _():
        signal(barrier, to_out)
        signal(barrier, to_in - core + 1)

    weights = [pltpu.make_async_copy(s, d, w_sem.at[i]) for i, (s, d) in enumerate(((wg, vwg), (wu, vwu), (wd, vwd)))]
    for w in weights:
        w.start()

    pl.semaphore_wait(barrier, jnp.where(is_end, 2, 3))

    def remote(src, dst, send, recv, device):
        return pltpu.make_async_remote_copy(
            src_ref=src, dst_ref=dst, send_sem=send, recv_sem=recv, device_id={"tp": device}, device_id_type=MESH
        )

    def x_part(b):
        j, h = b // HALVES, lax.rem(b, HALVES)
        return x.at[pl.ds(pl.multiple_of(j * rows, rows), rows), pl.ds(pl.multiple_of(h * half, half), half)]

    def own_to_in(b):
        slot = jnp.where(is_end, 0, PARTS) + b
        return remote(x_part(b), tm.at[slot], ti_send, tm_recv.at[slot], to_in)

    def own_to_out(b):
        return remote(x_part(b), tm.at[b], te_send, tm_recv.at[b], to_out)

    def own_to_sibling(b):
        return remote(x_part(b), ts.at[b], ts_send, ts_recv.at[0], sibling)

    def on_to_in(b):
        slot = 2 * PARTS + b
        return remote(tm.at[b], tm.at[slot], ti_send, tm_recv.at[slot], to_in)

    def on_to_out(a):
        return remote(tm.at[a], tm.at[a], te_send, tm_recv.at[a], to_out)

    def on_to_sibling(a):
        return remote(tm.at[a], ts.at[PARTS + a], ts_send, ts_recv.at[1 + a], sibling)

    def wait_arrival(a):
        on_to_out(a).wait_recv()

    def wait_bytes(ref, count, sem):
        whole = ref.at[pl.ds(0, count)]
        pltpu.make_async_copy(whole, whole, sem).wait()

    def loads(c, h, mine):
        theirs = ts.at[c * HALVES + h]
        return (
            pltpu.make_async_copy(mine, xb.at[h, pl.ds(0, rows)], x_sem.at[2 * h]),
            pltpu.make_async_copy(theirs, xb.at[h, pl.ds(rows, rows)], x_sem.at[2 * h + 1]),
        )

    def load_start(c, h):
        part = (c - CHUNKS) * HALVES + h
        ours, other = loads(c, h, tm.at[part])
        ours.start()
        on_to_sibling(part).wait_recv()
        other.start()

    def load_wait(c, h):
        for copy in loads(c, h, tm.at[0]):
            copy.wait()

    def load_arrived(c, h):
        load_start(c, h)
        load_wait(c, h)

    def product(weight, columns, h):
        return jnp.dot(xb[h], weight[pl.ds(h * half, half), columns], preferred_element_type=F32)

    def finish(c, columns, gate, up):
        hid[c, :, columns] = (jax.nn.gelu(gate) * up).astype(BF16)

    def hidden_tile(c, i):
        columns = pl.ds(pl.multiple_of(i * tile, tile), tile)
        gate = product(vwg, columns, 0) + product(vwg, columns, 1)
        up = product(vwu, columns, 0) + product(vwu, columns, 1)
        finish(c, columns, gate, up)

    def hidden_first():
        @pl.loop(0, tiles)
        def _(i):
            columns = pl.ds(pl.multiple_of(i * tile, tile), tile)
            acc[0, :, columns] = product(vwg, columns, 0)
            acc[1, :, columns] = product(vwu, columns, 0)

    def hidden_second(c):
        @pl.loop(0, tiles)
        def _(i):
            columns = pl.ds(pl.multiple_of(i * tile, tile), tile)
            gate = acc[0, :, columns] + product(vwg, columns, 1)
            up = acc[1, :, columns] + product(vwu, columns, 1)
            finish(c, columns, gate, up)

    def to_sibling(stg, sib, send, recv, k):
        s = lax.rem(k, RING)
        return remote(stg.at[s], sib.at[s], send.at[s], recv.at[s], sibling)

    def term(flow, k, c, n):
        own, sib, stg, send, recv = flow
        s = lax.rem(k, RING)

        @pl.when(k >= RING)
        def _():
            to_sibling(stg, sib, send, recv, k).wait_send()

        columns = pl.ds(pl.multiple_of(n * width, width), width)
        both = jnp.dot(hid[c], vwd[:, columns], preferred_element_type=F32)
        stg[s] = both[rows:].astype(BF16)
        own[s] = both[:rows]
        to_sibling(stg, sib, send, recv, k).start()

    def chip_sum(flow, k):
        own, sib, stg, send, recv = flow
        s = lax.rem(k, RING)
        to_sibling(stg, sib, send, recv, k).wait_recv()
        return own[s] + sib[s].astype(F32)

    def drain(flow):
        own, sib, stg, send, recv = flow

        @pl.loop(0, RING)
        def _(k):
            to_sibling(stg, sib, send, recv, k).wait_send()

    flow1 = (own1, sib1, stg1, d1_send, d1_recv)
    flow2 = (own2, sib2, stg2, d2_send, d2_recv)

    def end_sum_in(k):
        return remote(rse.at[k], rse.at[k], rse_send, rse_recv.at[jnp.maximum(k - EARLY + 1, 0)], to_in)

    def inner_sum_in(k):
        return remote(rse.at[k], rsi.at[k - UNIT], rse_send, rsi_recv.at[k - UNIT], to_in)

    def sum_out(k):
        return remote(rsi.at[k], rsi.at[k], rsi_send, rsi_recv.at[k], to_out)

    def result(k, total):
        j, n = lax.rem(k, UNIT) // PIECES, lax.rem(k, PIECES)
        y[pl.ds(pl.multiple_of(j * rows, rows), rows), pl.ds(pl.multiple_of(n * width, width), width)] = total.astype(BF16)

    def order(k, held, units):
        first = UNIT - held
        rest = units * UNIT - held
        return jnp.where(k < first, k, jnp.where(k < rest, k + held, k - rest + first))

    def all_parts(copy):
        for b in range(PARTS):
            copy(b).start()

    is_inner = jnp.logical_not(is_end)

    @pl.when(jnp.logical_or(is_end, core == 1))
    def _():
        all_parts(own_to_in)

    @pl.when(jnp.logical_and(is_inner, core == 0))
    def _():
        all_parts(own_to_out)

    @pl.when(is_inner)
    def _():
        signal(ready, sibling)

    all_parts(own_to_sibling)

    @pl.when(is_inner)
    def _():
        pl.semaphore_wait(ready, 1)

    @pl.when(jnp.logical_and(is_inner, core == 0))
    def _():
        all_parts(own_to_in)

    @pl.when(jnp.logical_and(is_inner, core == 1))
    def _():
        all_parts(own_to_out)

    weights[0].wait()
    weights[1].wait()

    wait_bytes(ts, PARTS, ts_recv.at[0])

    @pl.loop(0, CHUNKS)
    def _(j):
        for h in range(HALVES):
            for copy in loads(j, h, x_part(j * HALVES + h)):
                copy.start()

        for h in range(HALVES):
            load_wait(j, h)

        @pl.loop(0, tiles)
        def _(i):
            hidden_tile(j, i)

    weights[2].wait()

    def end_pieces(start, stop):
        @pl.loop(start, stop + AHEAD)
        def _(k):
            @pl.when(k < stop)
            def _():
                piece = order(k, HELD_END, 3)
                term(flow1, k, CHUNKS + piece // PIECES, lax.rem(piece, PIECES))

            @pl.when(k >= start + AHEAD)
            def _():
                piece = order(k - AHEAD, HELD_END, 3)
                rse[piece] = chip_sum(flow1, k - AHEAD).astype(BF16)
                end_sum_in(piece).start()

    def straight_to_sibling(a, h):
        return remote(tm.at[a], xb.at[h, pl.ds(rows, rows)], ts_send, ts_recv.at[1 + a], sibling)

    @pl.when(is_end)
    def _():
        for h in range(HALVES):
            pl.semaphore_signal(free.at[h], inc=1, device_id={"tp": sibling}, device_id_type=MESH)

        @pl.loop(0, 3 * CHUNKS)
        def _(a):
            c = CHUNKS + a
            for h in range(HALVES):
                part = a * HALVES + h
                wait_arrival(part)
                ours = pltpu.make_async_copy(tm.at[part], xb.at[h, pl.ds(0, rows)], x_sem.at[2 * h])
                ours.start()
                pl.semaphore_wait(free.at[h], 1)
                straight = straight_to_sibling(part, h)
                straight.start()
                ours.wait()
                straight.wait_recv()
                if h == 0:
                    hidden_first()
                else:
                    hidden_second(c)

                @pl.when(a < 3 * CHUNKS - 1)
                def _(h=h):
                    pl.semaphore_signal(free.at[h], inc=1, device_id={"tp": sibling}, device_id_type=MESH)

            start = a * PIECES - jnp.where(a >= CHUNKS, HELD_END, 0)
            stop = (a + 1) * PIECES - jnp.where(a >= CHUNKS - 1, HELD_END, 0)
            end_pieces(start, stop)

        end_pieces(3 * UNIT - HELD_END, 3 * UNIT)

        @pl.loop(0, UNIT + AHEAD)
        def _(k):
            @pl.when(k < UNIT)
            def _():
                term(flow2, k, k // PIECES, lax.rem(k, PIECES))

            @pl.when(k >= AHEAD)
            def _():
                q = k - AHEAD
                total = chip_sum(flow2, q)
                sum_out(UNIT + q).wait_recv()
                result(q, total + rsi[UNIT + q].astype(F32))

        wait_bytes(rse, 3 * UNIT, rse_send)
        wait_bytes(tm, PARTS, ti_send)

    @pl.when(jnp.logical_not(is_end))
    def _():
        def inner_arrivals(j, h):
            b = j * HALVES + h
            wait_arrival(b)
            on_to_in(b).start()
            on_to_sibling(b).start()
            wait_arrival(PARTS + b)
            on_to_out(PARTS + b).start()
            on_to_sibling(PARTS + b).start()

        def far(j, h):
            a = 2 * PARTS + j * HALVES + h
            wait_arrival(a)
            on_to_out(a).start()
            on_to_sibling(a).start()

        @pl.loop(0, CHUNKS)
        def _(j):
            inner_arrivals(j, 0)
            load_arrived(CHUNKS + j, 0)
            hidden_first()
            inner_arrivals(j, 1)
            load_arrived(CHUNKS + j, 1)
            hidden_second(CHUNKS + j)
            load_start(2 * CHUNKS + j, 0)
            load_start(2 * CHUNKS + j, 1)
            load_wait(2 * CHUNKS + j, 0)
            load_wait(2 * CHUNKS + j, 1)

            @pl.loop(0, tiles)
            def _(i):
                hidden_tile(2 * CHUNKS + j, i)

        far(0, 0)
        load_arrived(3 * CHUNKS, 0)
        hidden_first()
        far(0, 1)
        load_arrived(3 * CHUNKS, 1)
        hidden_second(3 * CHUNKS)
        last = 4 * CHUNKS - 1

        def term1(k):
            piece = order(k, HELD_INNER, 2)
            term(flow1, k, 2 * CHUNKS + piece // PIECES, lax.rem(piece, PIECES))

        def place2(p):
            first, rest = UNIT - HELD, 2 * UNIT - HELD_INNER
            piece = jnp.where(p < first, p, jnp.where(p < rest, p + HELD_INNER, p - rest + first))
            count = jnp.where(p < first, p, p - (HELD - HELD_INNER))
            return piece, count, jnp.logical_or(p < first, p >= UNIT - HELD_INNER)

        stop2 = 2 * UNIT - HELD_INNER + HELD

        def term2(p):
            piece, count, present = place2(p)

            @pl.when(jnp.logical_and(present, jnp.logical_and(p >= 0, p < stop2)))
            def _():
                term(flow2, count, piece // PIECES, lax.rem(piece, PIECES))

        for k in range(NEXT):
            term1(k)

        for k in range(NEXT - LAG):
            term2(k)

        @pl.loop(0, stop2 + LAG)
        def _(p):
            @pl.when(p < 2 * UNIT)
            def _():
                k = UNIT + order(p, HELD_INNER, 2)
                total = chip_sum(flow1, p)
                end_sum_in(k).wait_recv()
                rse[k] = (total + rse[k].astype(F32)).astype(BF16)
                inner_sum_in(k).start()

            @pl.when(p < 2 * UNIT - NEXT)
            def _():
                term1(p + NEXT)

            q, count, present = place2(p - LAG)

            @pl.when(jnp.logical_and(p >= LAG, present))
            def _():
                total = chip_sum(flow2, count)
                sum_out(q).wait_recv()
                total = total + rsi[q].astype(F32)

                @pl.when(q == 0)
                def _():
                    wait_bytes(rse, EARLY, rse_recv.at[0])

                @pl.when(jnp.logical_and(q >= EARLY, q < UNIT))
                def _():
                    end_sum_in(q).wait_recv()

                @pl.when(q < UNIT)
                def _():
                    result(q, total + rse[q].astype(F32))

                @pl.when(q >= UNIT)
                def _():
                    rsi[q] = total.astype(BF16)
                    sum_out(q).start()

            term2(p - LAG + NEXT)

            @pl.when(p == FAR)
            def _():
                far(1, 0)
                far(1, 1)

            @pl.when(p == FAR + 2)
            def _():
                load_start(last, 0)
                load_start(last, 1)

            @pl.when(p == FAR + 3)
            def _():
                load_wait(last, 0)
                load_wait(last, 1)

            @pl.when(jnp.logical_and(p >= FAR + 3, p < FAR + 3 + tiles))
            def _():
                hidden_tile(last, p - FAR - 3)

        wait_bytes(rse, 2 * UNIT, rse_send)
        wait_bytes(rsi, UNIT, rsi_send)
        wait_bytes(tm, 2 * PARTS, ti_send)
        wait_bytes(tm, 3 * PARTS, te_send)

    drain(flow1)
    drain(flow2)
    wait_bytes(ts, 4 * PARTS, ts_send)


def solution(mesh):
    def step(x, w_gate, w_up, w_down):
        n_rows, d = x.shape
        ff = w_gate.shape[1]
        rows, width = n_rows // CHUNKS, d // PIECES
        dma = pltpu.SemaphoreType.DMA
        out, _, _ = pl.pallas_call(
            kernel,
            out_shape=[
                pltpu.VMEM((n_rows, d), BF16),
                jax.ShapeDtypeStruct((3 * PARTS, rows, d // HALVES), BF16),
                jax.ShapeDtypeStruct((4 * PARTS, rows, d // HALVES), BF16),
            ],
            in_specs=[pl.BlockSpec(memory_space=pltpu.HBM)] * 4,
            out_specs=[pl.BlockSpec(memory_space=pltpu.VMEM)] + [pl.BlockSpec(memory_space=pltpu.HBM)] * 2,
            scratch_shapes=[
                pltpu.VMEM((d, ff), BF16),
                pltpu.VMEM((d, ff), BF16),
                pltpu.VMEM((ff, d), BF16),
                pltpu.VMEM((HALVES, 2 * rows, d // HALVES), BF16),
                pltpu.VMEM((2, 2 * rows, ff), F32),
                pltpu.VMEM((4 * CHUNKS, 2 * rows, ff), BF16),
                *[
                    pltpu.VMEM((RING, rows, width), F32),
                    pltpu.VMEM((RING, rows, width), BF16),
                    pltpu.VMEM((RING, rows, width), BF16),
                ]
                * 2,
                pltpu.VMEM((3 * UNIT, rows, width), BF16),
                pltpu.VMEM((2 * UNIT, rows, width), BF16),
                pltpu.SemaphoreType.REGULAR,
                pltpu.SemaphoreType.REGULAR((HALVES,)),
                dma((3,)),
                dma((2 * HALVES,)),
                dma((3 * PARTS,)),
                dma((3 * PARTS + 1,)),
                dma,
                dma,
                dma,
                dma((RING,)),
                dma((RING,)),
                dma((RING,)),
                dma((RING,)),
                dma,
                dma((3 * UNIT - EARLY + 1,)),
                dma,
                dma((2 * UNIT,)),
            ],
            compiler_params=pltpu.CompilerParams(
                collective_id=0, has_side_effects=True, vmem_limit_bytes=64_000_000
            ),
            name="mlp_line",
        )(x, w_gate, w_up, w_down)
        return out

    return jax.shard_map(
        step,
        mesh=mesh,
        in_specs=(P(("dp", "tp"), None), P(None, "tp"), P(None, "tp"), P("tp", None)),
        out_specs=P(("dp", "tp"), None),
        check_vma=False,
    )
```

```python
import functools

import jax
import jax.numpy as jnp
from jax import lax
from jax.experimental import pallas as pl
from jax.experimental.pallas import tpu as pltpu
from jax.sharding import PartitionSpec as P

MESH = pl.DeviceIdType.MESH
F32, BF16 = jnp.float32, jnp.bfloat16

CHUNKS = 2
HALVES = 2
PARTS = CHUNKS * HALVES
PIECES = 8
RING = 4
AHEAD = 1
NEXT = 2
LAG = 2
HELD_END, HELD_INNER = 4, 2
UNIT = CHUNKS * PIECES
HELD = max(HELD_END, HELD_INNER)
EARLY = UNIT - HELD
FAR = 3


def kernel(
    x, wg, wu, wd, y, tm, ts, vwg, vwu, vwd, xb, acc, hid,
    own1, sib1, stg1, own2, sib2, stg2, rse, rsi,
    ready, free, w_sem, x_sem, tm_recv, ts_recv, ti_send, te_send, ts_send,
    d1_send, d1_recv, d2_send, d2_recv, rse_send, rse_recv, rsi_send, rsi_recv,
):
    me = lax.axis_index("tp")
    chip, core = me // 2, lax.rem(me, 2)
    is_end = jnp.logical_or(chip == 0, chip == 3)
    sibling = me + 1 - 2 * core
    inward = jnp.where(chip < 2, 2, -2)
    to_in, to_out = me + inward, me - inward
    rows, half = x.shape[0] // CHUNKS, x.shape[1] // HALVES
    width = y.shape[1] // PIECES
    tile = min(256, vwg.shape[1])
    tiles = vwg.shape[1] // tile

    barrier = pltpu.get_barrier_semaphore()
    def signal(semaphore, device):
        pl.semaphore_signal(semaphore, inc=1, device_id={"tp": device}, device_id_type=MESH)

    signal(barrier, sibling)

    @pl.when(is_end)
    def _():
        signal(barrier, to_in - core + 1)

    @pl.when(jnp.logical_not(is_end))
    def _():
        signal(barrier, to_out)
        signal(barrier, to_in - core)

    weights = [pltpu.make_async_copy(s, d, w_sem.at[i]) for i, (s, d) in enumerate(((wg, vwg), (wu, vwu), (wd, vwd)))]
    for w in weights:
        w.start()

    pl.semaphore_wait(barrier, jnp.where(is_end, 2, 3))

    def remote(src, dst, send, recv, device):
        return pltpu.make_async_remote_copy(
            src_ref=src, dst_ref=dst, send_sem=send, recv_sem=recv, device_id={"tp": device}, device_id_type=MESH
        )

    def x_part(b):
        j, h = b // HALVES, lax.rem(b, HALVES)
        return x.at[pl.ds(pl.multiple_of(j * rows, rows), rows), pl.ds(pl.multiple_of(h * half, half), half)]

    def own_to_in(b):
        slot = jnp.where(is_end, 0, PARTS) + b
        return remote(x_part(b), tm.at[slot], ti_send, tm_recv.at[slot], to_in)

    def own_to_out(b):
        return remote(x_part(b), tm.at[b], te_send, tm_recv.at[b], to_out)

    def own_to_sibling(b):
        return remote(x_part(b), ts.at[b], ts_send, ts_recv.at[0], sibling)

    def on_to_in(b):
        slot = 2 * PARTS + b
        return remote(tm.at[b], tm.at[slot], ti_send, tm_recv.at[slot], to_in)

    def on_to_out(a):
        return remote(tm.at[a], tm.at[a], te_send, tm_recv.at[a], to_out)

    def on_to_sibling(a):
        return remote(tm.at[a], ts.at[PARTS + a], ts_send, ts_recv.at[1 + a], sibling)

    def wait_arrival(a):
        on_to_out(a).wait_recv()

    def wait_bytes(ref, count, sem):
        whole = ref.at[pl.ds(0, count)]
        pltpu.make_async_copy(whole, whole, sem).wait()

    def loads(c, h, mine):
        theirs = ts.at[c * HALVES + h]
        return (
            pltpu.make_async_copy(mine, xb.at[h, pl.ds(0, rows)], x_sem.at[2 * h]),
            pltpu.make_async_copy(theirs, xb.at[h, pl.ds(rows, rows)], x_sem.at[2 * h + 1]),
        )

    def load_start(c, h):
        part = (c - CHUNKS) * HALVES + h
        ours, other = loads(c, h, tm.at[part])
        ours.start()
        on_to_sibling(part).wait_recv()
        other.start()

    def load_wait(c, h):
        for copy in loads(c, h, tm.at[0]):
            copy.wait()

    def load_arrived(c, h):
        load_start(c, h)
        load_wait(c, h)

    def product(weight, columns, h):
        return jnp.dot(xb[h], weight[pl.ds(h * half, half), columns], preferred_element_type=F32)

    def finish(c, columns, gate, up):
        hid[c, :, columns] = (jax.nn.gelu(gate) * up).astype(BF16)

    def hidden_tile(c, i):
        columns = pl.ds(pl.multiple_of(i * tile, tile), tile)
        gate = product(vwg, columns, 0) + product(vwg, columns, 1)
        up = product(vwu, columns, 0) + product(vwu, columns, 1)
        finish(c, columns, gate, up)

    def hidden_first():
        @pl.loop(0, tiles)
        def _(i):
            columns = pl.ds(pl.multiple_of(i * tile, tile), tile)
            acc[0, :, columns] = product(vwg, columns, 0)
            acc[1, :, columns] = product(vwu, columns, 0)

    def hidden_second(c):
        @pl.loop(0, tiles)
        def _(i):
            columns = pl.ds(pl.multiple_of(i * tile, tile), tile)
            gate = acc[0, :, columns] + product(vwg, columns, 1)
            up = acc[1, :, columns] + product(vwu, columns, 1)
            finish(c, columns, gate, up)

    def to_sibling(stg, sib, send, recv, k):
        s = lax.rem(k, RING)
        return remote(stg.at[s], sib.at[s], send.at[s], recv.at[s], sibling)

    def term(flow, k, c, n):
        own, sib, stg, send, recv = flow
        s = lax.rem(k, RING)

        @pl.when(k >= RING)
        def _():
            to_sibling(stg, sib, send, recv, k).wait_send()

        columns = pl.ds(pl.multiple_of(n * width, width), width)
        both = jnp.dot(hid[c], vwd[:, columns], preferred_element_type=F32)
        stg[s] = both[rows:].astype(BF16)
        own[s] = both[:rows]
        to_sibling(stg, sib, send, recv, k).start()

    def chip_sum(flow, k):
        own, sib, stg, send, recv = flow
        s = lax.rem(k, RING)
        to_sibling(stg, sib, send, recv, k).wait_recv()
        return own[s] + sib[s].astype(F32)

    def drain(flow):
        own, sib, stg, send, recv = flow

        @pl.loop(0, RING)
        def _(k):
            to_sibling(stg, sib, send, recv, k).wait_send()

    flow1 = (own1, sib1, stg1, d1_send, d1_recv)
    flow2 = (own2, sib2, stg2, d2_send, d2_recv)

    def end_sum_in(k):
        return remote(rse.at[k], rse.at[k], rse_send, rse_recv.at[jnp.maximum(k - EARLY + 1, 0)], to_in)

    def inner_sum_in(k):
        return remote(rse.at[k], rsi.at[k - UNIT], rse_send, rsi_recv.at[k - UNIT], to_in)

    def sum_out(k):
        return remote(rsi.at[k], rsi.at[k], rsi_send, rsi_recv.at[k], to_out)

    def result(k, total):
        j, n = lax.rem(k, UNIT) // PIECES, lax.rem(k, PIECES)
        y[pl.ds(pl.multiple_of(j * rows, rows), rows), pl.ds(pl.multiple_of(n * width, width), width)] = total.astype(BF16)

    def order(k, held, units):
        first = UNIT - held
        rest = units * UNIT - held
        return jnp.where(k < first, k, jnp.where(k < rest, k + held, k - rest + first))

    def all_parts(copy):
        for b in range(PARTS):
            copy(b).start()

    is_inner = jnp.logical_not(is_end)

    @pl.when(jnp.logical_or(is_end, core == 0))
    def _():
        all_parts(own_to_in)

    @pl.when(jnp.logical_and(is_inner, core == 1))
    def _():
        all_parts(own_to_out)

    @pl.when(is_inner)
    def _():
        signal(ready, sibling)

    all_parts(own_to_sibling)

    @pl.when(is_inner)
    def _():
        pl.semaphore_wait(ready, 1)

    @pl.when(jnp.logical_and(is_inner, core == 1))
    def _():
        all_parts(own_to_in)

    @pl.when(jnp.logical_and(is_inner, core == 0))
    def _():
        all_parts(own_to_out)

    weights[0].wait()
    weights[1].wait()

    wait_bytes(ts, PARTS, ts_recv.at[0])

    @pl.loop(0, CHUNKS)
    def _(j):
        for h in range(HALVES):
            for copy in loads(j, h, x_part(j * HALVES + h)):
                copy.start()

        for h in range(HALVES):
            load_wait(j, h)

        @pl.loop(0, tiles)
        def _(i):
            hidden_tile(j, i)

    weights[2].wait()

    def end_pieces(start, stop):
        @pl.loop(start, stop + AHEAD)
        def _(k):
            @pl.when(k < stop)
            def _():
                piece = order(k, HELD_END, 3)
                term(flow1, k, CHUNKS + piece // PIECES, lax.rem(piece, PIECES))

            @pl.when(k >= start + AHEAD)
            def _():
                piece = order(k - AHEAD, HELD_END, 3)
                rse[piece] = chip_sum(flow1, k - AHEAD).astype(BF16)
                end_sum_in(piece).start()

    def straight_to_sibling(a, h):
        return remote(tm.at[a], xb.at[h, pl.ds(rows, rows)], ts_send, ts_recv.at[1 + a], sibling)

    @pl.when(is_end)
    def _():
        for h in range(HALVES):
            pl.semaphore_signal(free.at[h], inc=1, device_id={"tp": sibling}, device_id_type=MESH)

        @pl.loop(0, 3 * CHUNKS)
        def _(a):
            c = CHUNKS + a
            for h in range(HALVES):
                part = a * HALVES + h
                wait_arrival(part)
                ours = pltpu.make_async_copy(tm.at[part], xb.at[h, pl.ds(0, rows)], x_sem.at[2 * h])
                ours.start()
                pl.semaphore_wait(free.at[h], 1)
                straight = straight_to_sibling(part, h)
                straight.start()
                ours.wait()
                straight.wait_recv()
                if h == 0:
                    hidden_first()
                else:
                    hidden_second(c)

                @pl.when(a < 3 * CHUNKS - 1)
                def _(h=h):
                    pl.semaphore_signal(free.at[h], inc=1, device_id={"tp": sibling}, device_id_type=MESH)

            start = a * PIECES - jnp.where(a >= CHUNKS, HELD_END, 0)
            stop = (a + 1) * PIECES - jnp.where(a >= CHUNKS - 1, HELD_END, 0)
            end_pieces(start, stop)

        end_pieces(3 * UNIT - HELD_END, 3 * UNIT)

        @pl.loop(0, UNIT + AHEAD)
        def _(k):
            @pl.when(k < UNIT)
            def _():
                term(flow2, k, k // PIECES, lax.rem(k, PIECES))

            @pl.when(k >= AHEAD)
            def _():
                q = k - AHEAD
                total = chip_sum(flow2, q)
                sum_out(UNIT + q).wait_recv()
                result(q, total + rsi[UNIT + q].astype(F32))

        wait_bytes(rse, 3 * UNIT, rse_send)
        wait_bytes(tm, PARTS, ti_send)

    @pl.when(jnp.logical_not(is_end))
    def _():
        def inner_arrivals(j, h):
            b = j * HALVES + h
            wait_arrival(b)
            on_to_in(b).start()
            on_to_sibling(b).start()
            wait_arrival(PARTS + b)
            on_to_out(PARTS + b).start()
            on_to_sibling(PARTS + b).start()

        def far(j, h):
            a = 2 * PARTS + j * HALVES + h
            wait_arrival(a)
            on_to_out(a).start()
            on_to_sibling(a).start()

        @pl.loop(0, CHUNKS)
        def _(j):
            inner_arrivals(j, 0)
            load_arrived(CHUNKS + j, 0)
            hidden_first()
            inner_arrivals(j, 1)
            load_arrived(CHUNKS + j, 1)
            hidden_second(CHUNKS + j)
            load_start(2 * CHUNKS + j, 0)
            load_start(2 * CHUNKS + j, 1)
            load_wait(2 * CHUNKS + j, 0)
            load_wait(2 * CHUNKS + j, 1)

            @pl.loop(0, tiles)
            def _(i):
                hidden_tile(2 * CHUNKS + j, i)

        far(0, 0)
        load_arrived(3 * CHUNKS, 0)
        hidden_first()
        far(0, 1)
        load_arrived(3 * CHUNKS, 1)
        hidden_second(3 * CHUNKS)
        last = 4 * CHUNKS - 1

        def term1(k):
            piece = order(k, HELD_INNER, 2)
            term(flow1, k, 2 * CHUNKS + piece // PIECES, lax.rem(piece, PIECES))

        def place2(p):
            first, rest = UNIT - HELD, 2 * UNIT - HELD_INNER
            piece = jnp.where(p < first, p, jnp.where(p < rest, p + HELD_INNER, p - rest + first))
            count = jnp.where(p < first, p, p - (HELD - HELD_INNER))
            return piece, count, jnp.logical_or(p < first, p >= UNIT - HELD_INNER)

        stop2 = 2 * UNIT - HELD_INNER + HELD

        def term2(p):
            piece, count, present = place2(p)

            @pl.when(jnp.logical_and(present, jnp.logical_and(p >= 0, p < stop2)))
            def _():
                term(flow2, count, piece // PIECES, lax.rem(piece, PIECES))

        for k in range(NEXT):
            term1(k)

        for k in range(NEXT - LAG):
            term2(k)

        @pl.loop(0, stop2 + LAG)
        def _(p):
            @pl.when(p < 2 * UNIT)
            def _():
                k = UNIT + order(p, HELD_INNER, 2)
                total = chip_sum(flow1, p)
                end_sum_in(k).wait_recv()
                rse[k] = (total + rse[k].astype(F32)).astype(BF16)
                inner_sum_in(k).start()

            @pl.when(p < 2 * UNIT - NEXT)
            def _():
                term1(p + NEXT)

            q, count, present = place2(p - LAG)

            @pl.when(jnp.logical_and(p >= LAG, present))
            def _():
                total = chip_sum(flow2, count)
                sum_out(q).wait_recv()
                total = total + rsi[q].astype(F32)

                @pl.when(q == 0)
                def _():
                    wait_bytes(rse, EARLY, rse_recv.at[0])

                @pl.when(jnp.logical_and(q >= EARLY, q < UNIT))
                def _():
                    end_sum_in(q).wait_recv()

                @pl.when(q < UNIT)
                def _():
                    result(q, total + rse[q].astype(F32))

                @pl.when(q >= UNIT)
                def _():
                    rsi[q] = total.astype(BF16)
                    sum_out(q).start()

            term2(p - LAG + NEXT)

            @pl.when(p == FAR)
            def _():
                far(1, 0)
                far(1, 1)

            @pl.when(p == FAR + 2)
            def _():
                load_start(last, 0)
                load_start(last, 1)

            @pl.when(p == FAR + 3)
            def _():
                load_wait(last, 0)
                load_wait(last, 1)

            @pl.when(jnp.logical_and(p >= FAR + 3, p < FAR + 3 + tiles))
            def _():
                hidden_tile(last, p - FAR - 3)

        wait_bytes(rse, 2 * UNIT, rse_send)
        wait_bytes(rsi, UNIT, rsi_send)
        wait_bytes(tm, 2 * PARTS, ti_send)
        wait_bytes(tm, 3 * PARTS, te_send)

    drain(flow1)
    drain(flow2)
    wait_bytes(ts, 4 * PARTS, ts_send)


def solution(mesh):
    def step(x, w_gate, w_up, w_down):
        n_rows, d = x.shape
        ff = w_gate.shape[1]
        rows, width = n_rows // CHUNKS, d // PIECES
        dma = pltpu.SemaphoreType.DMA
        out, _, _ = pl.pallas_call(
            kernel,
            out_shape=[
                pltpu.VMEM((n_rows, d), BF16),
                jax.ShapeDtypeStruct((3 * PARTS, rows, d // HALVES), BF16),
                jax.ShapeDtypeStruct((4 * PARTS, rows, d // HALVES), BF16),
            ],
            in_specs=[pl.BlockSpec(memory_space=pltpu.HBM)] * 4,
            out_specs=[pl.BlockSpec(memory_space=pltpu.VMEM)] + [pl.BlockSpec(memory_space=pltpu.HBM)] * 2,
            scratch_shapes=[
                pltpu.VMEM((d, ff), BF16),
                pltpu.VMEM((d, ff), BF16),
                pltpu.VMEM((ff, d), BF16),
                pltpu.VMEM((HALVES, 2 * rows, d // HALVES), BF16),
                pltpu.VMEM((2, 2 * rows, ff), F32),
                pltpu.VMEM((4 * CHUNKS, 2 * rows, ff), BF16),
                *[
                    pltpu.VMEM((RING, rows, width), F32),
                    pltpu.VMEM((RING, rows, width), BF16),
                    pltpu.VMEM((RING, rows, width), BF16),
                ]
                * 2,
                pltpu.VMEM((3 * UNIT, rows, width), BF16),
                pltpu.VMEM((2 * UNIT, rows, width), BF16),
                pltpu.SemaphoreType.REGULAR,
                pltpu.SemaphoreType.REGULAR((HALVES,)),
                dma((3,)),
                dma((2 * HALVES,)),
                dma((3 * PARTS,)),
                dma((3 * PARTS + 1,)),
                dma,
                dma,
                dma,
                dma((RING,)),
                dma((RING,)),
                dma((RING,)),
                dma((RING,)),
                dma,
                dma((3 * UNIT - EARLY + 1,)),
                dma,
                dma((2 * UNIT,)),
            ],
            compiler_params=pltpu.CompilerParams(
                collective_id=0, has_side_effects=True, vmem_limit_bytes=64_000_000
            ),
            name="mlp_line",
        )(x, w_gate, w_up, w_down)
        return out

    return jax.shard_map(
        step,
        mesh=mesh,
        in_specs=(P(("dp", "tp"), None), P(None, "tp"), P(None, "tp"), P("tp", None)),
        out_specs=P(("dp", "tp"), None),
        check_vma=False,
    )
```
